32 devices in a mesh: seq: 8 (over z, y), head: 4 (over x, core).
Axes of the slice: x: 2, y: 2, z: 4, core: 2. Of those that a mesh axis runs over, the one named last changes fastest.
Arguments:
- queries: bfloat16 [1024, 24576], P('seq', 'head'), may hold values from -325 to 325
- latents: bfloat16 [1024, 576], P('seq'), may hold values from -5 to 5
- doc_ids: int32 [1024], P('seq'), may hold values from 0 to 3, never falling along the last dimension, each value on 1 to 512 neighbouring positions
- key_weight: bfloat16 [512, 16384], P(None, 'head'), may hold values from -0.25 to 0.25
- value_weight: bfloat16 [512, 16384], P(None, 'head'), may hold values from -0.25 to 0.25
- out_grad: bfloat16 [1024, 16384], P('seq', 'head'), may hold values from -6 to 6
Outputs:
- attended: bfloat16 [1024, 16384], P('seq', 'head')
- latent_grad: float32 [1024, 576], P('seq')
- key_weight_grad: float32 [512, 16384], P('seq', 'head')
- value_weight_grad: float32 [512, 16384], P('seq', 'head')
The draws below stay inside these ranges and needn't reach their ends.
Inputs may be any that keep to these rules, and one draw needn't show every extreme that they name: `doc_ids`: ids never fall along the sequence; every document holds 1 to 512 tokens, and one holds exactly that many.
All inputs are finite; a program needn't handle non-finite values.
Results may differ from the reference program's by a relative error of at most 0.028.
Values may be sent and summed in bfloat16 or wider, within the bound.
A program may use at most 128 MiB of HBM per device.

```python
import math
import jax
import jax.numpy as jnp
import numpy as np
from jax import lax

HEADS = 128
NOPE = 128
ROPE = 64
VDIM = 128
LATENT = 512
TOK_DEV = 128
REACH = 4
TOKENS = 1024
DOCS = 4


def base_latents(key):
    normal_rows = jax.random.normal(jax.random.fold_in(key, 7), (TOKENS, LATENT + ROPE), jnp.float32)
    return jnp.clip(normal_rows, -5.0, 5.0)


def draw_latents(key, part):
    drawn = base_latents(key)
    return drawn.astype(jnp.bfloat16)


def draw_queries(key, part):
    width = NOPE + ROPE
    drawn = jax.random.normal(jax.random.fold_in(key, 3), (TOKENS, HEADS, width), jnp.float32)
    drawn = jnp.clip(drawn, -5.0, 5.0)
    return drawn.reshape(TOKENS, HEADS * width).astype(jnp.bfloat16)


def shard_levels(stream_key, dims, shards, low, high):
    level = 1.0
    for dim, parts in shards:
        steps = jax.random.uniform(jax.random.fold_in(jax.random.fold_in(stream_key, 6), dim), (parts,), jnp.float32, low / len(shards), high / len(shards))
        level = level * jnp.repeat(jnp.exp(steps), dims[dim] // parts).reshape((-1,) + (1,) * (len(dims) - 1 - dim))
    return level


def split_up(count, total, limit, lean):
    weights = [(1 << 20) // math.isqrt(standing ** lean) + 1 for standing in range(2, count + 1)]
    rest, given = total - limit - (count - 1), [1] * (count - 1)
    while rest > 0:
        movable = [i for i in range(count - 1) if given[i] < limit]
        pool, budget = sum([weights[i] for i in movable]), rest
        for i in movable:
            more = min(limit - given[i], max(1, budget * weights[i] // pool), rest)
            given[i] = given[i] + more
            rest = rest - more
    return np.array([limit] + given)


def ragged_sizes(own_key, number_of, total, reach, lean):
    if number_of == 2:
        one = jax.random.randint(own_key, (), max(1, total - reach), min(reach, total - 1) + 1)
        return jnp.stack([one, total - one])
    sizes = jnp.asarray(split_up(number_of, total, reach, lean), jnp.int32)
    pairs = (number_of - 1) // 2
    giver, taker = sizes[1:1 + 2 * pairs:2], sizes[2:2 + 2 * pairs:2]
    room = jnp.minimum(giver - 1, reach - taker)
    passed = jax.random.randint(jax.random.fold_in(own_key, 1), (pairs,), 0, 1 << 20) % (room + 1)
    sizes = sizes.at[1:1 + 2 * pairs:2].set(giver - passed).at[2:2 + 2 * pairs:2].set(taker + passed)
    return sizes[jax.random.permutation(jax.random.fold_in(own_key, 2), number_of)]


def normal_values(own_key, extent, deviation, bound, split=(), held_as=jnp.bfloat16):
    factor_of = shard_levels(own_key, extent, split, -0.22, 0.18) if split else 1.0
    values = jax.random.normal(own_key, extent, jnp.float32) * deviation * factor_of
    return jnp.minimum(jnp.maximum(values, -bound), bound).astype(held_as)


def setup_inputs(seed: int = 0) -> dict:
    seeds = jax.random.split(jax.random.key(seed), 7)
    queries = draw_queries(jax.random.fold_in(seeds[6], 71), 0)
    latents = draw_latents(jax.random.fold_in(seeds[6], 71), 0)
    doc_ids = jnp.searchsorted(jnp.cumsum(ragged_sizes(seeds[2], DOCS, TOKENS, REACH * TOK_DEV, 1)), jnp.arange(TOKENS), side="right").astype(jnp.int32)
    key_weight = normal_values(seeds[3], (LATENT, HEADS * NOPE), LATENT ** -0.5, 0.25, ((1, 4),))
    value_weight = normal_values(seeds[4], (LATENT, HEADS * VDIM), LATENT ** -0.5, 0.25, ((1, 4),))
    out_grad = normal_values(seeds[5], (TOKENS, HEADS * VDIM), 1.0, 6.0, ((0, 8), (1, 4)))
    return {"queries": queries, "latents": latents, "doc_ids": doc_ids, "key_weight": key_weight, "value_weight": value_weight, "out_grad": out_grad}


def reference(queries, latents, doc_ids, key_weight, value_weight, out_grad):
    query_width = NOPE + ROPE
    score_scale = 1.0 / (query_width ** 0.5)
    block_count = TOKENS // TOK_DEV
    key_rows = (REACH + 1) * TOK_DEV
    lead_rows = REACH * TOK_DEV
    latent_part = latents[:, :LATENT]
    k_nope = jnp.dot(latent_part, key_weight, preferred_element_type=jnp.float32).astype(jnp.bfloat16)
    values_up = jnp.dot(latent_part, value_weight, preferred_element_type=jnp.float32).astype(jnp.bfloat16)
    nope_pad = jnp.concatenate([jnp.zeros((lead_rows, HEADS * NOPE), jnp.bfloat16), k_nope], axis=0)
    value_pad = jnp.concatenate([jnp.zeros((lead_rows, HEADS * VDIM), jnp.bfloat16), values_up], axis=0)
    rope_pad = jnp.concatenate([jnp.zeros((lead_rows, ROPE), jnp.bfloat16), latents[:, LATENT:]], axis=0)
    latent_pad = jnp.concatenate([jnp.zeros((lead_rows, LATENT), jnp.bfloat16), latent_part], axis=0)
    ids_pad = jnp.concatenate([jnp.full((lead_rows,), -1, jnp.int32), doc_ids.astype(jnp.int32)], axis=0)
    pos_pad = jnp.arange(TOKENS + lead_rows, dtype=jnp.int32) - lead_rows

    def block_step(totals, block_index):
        first_row = (block_index * TOK_DEV).astype(jnp.int32)
        query_heads = lax.dynamic_slice_in_dim(queries, first_row, TOK_DEV, 0).reshape(TOK_DEV, HEADS, query_width).astype(jnp.float32)
        grad_heads = lax.dynamic_slice_in_dim(out_grad, first_row, TOK_DEV, 0).reshape(TOK_DEV, HEADS, VDIM).astype(jnp.float32)
        query_ids = lax.dynamic_slice_in_dim(doc_ids.astype(jnp.int32), first_row, TOK_DEV, 0)
        query_pos = first_row + jnp.arange(TOK_DEV, dtype=jnp.int32)
        key_heads = lax.dynamic_slice_in_dim(nope_pad, first_row, key_rows, 0)
        value_heads = lax.dynamic_slice_in_dim(value_pad, first_row, key_rows, 0)
        key_rope = lax.dynamic_slice_in_dim(rope_pad, first_row, key_rows, 0).astype(jnp.float32)
        latent_rows = lax.dynamic_slice_in_dim(latent_pad, first_row, key_rows, 0)
        key_ids = lax.dynamic_slice_in_dim(ids_pad, first_row, key_rows, 0)
        key_pos = lax.dynamic_slice_in_dim(pos_pad, first_row, key_rows, 0)
        key_f = key_heads.reshape(key_rows, HEADS, NOPE).astype(jnp.float32)
        value_f = value_heads.reshape(key_rows, HEADS, VDIM).astype(jnp.float32)
        scores = jnp.einsum("phd,thd->hpt", query_heads[:, :, :NOPE], key_f, precision=lax.Precision.HIGHEST)
        scores = scores + jnp.einsum("phr,tr->hpt", query_heads[:, :, NOPE:], key_rope, precision=lax.Precision.HIGHEST)
        scores = scores * score_scale
        visible = (key_pos[None, :] <= query_pos[:, None]) & (key_ids[None, :] == query_ids[:, None])
        scores = jnp.where(visible[None], scores, -jnp.inf)
        row_top = jnp.max(scores, axis=-1, keepdims=True)
        row_lse = row_top + jnp.log(jnp.sum(jnp.exp(scores - row_top), axis=-1, keepdims=True))
        weight_f = jnp.exp(scores - row_lse)
        weight_b = weight_f.astype(jnp.bfloat16)
        output = jnp.einsum("hpt,thd->phd", weight_b.astype(jnp.float32), value_f, precision=lax.Precision.HIGHEST).astype(jnp.bfloat16)
        d_weight = jnp.einsum("phd,thd->hpt", grad_heads, value_f, precision=lax.Precision.HIGHEST)
        row_delta = jnp.sum(grad_heads * output.astype(jnp.float32), axis=-1)
        d_score = (weight_f * (d_weight - jnp.transpose(row_delta)[:, :, None]) * score_scale).astype(jnp.bfloat16)
        d_key = jnp.einsum("hpt,phd->thd", d_score.astype(jnp.float32), query_heads, precision=lax.Precision.HIGHEST).astype(jnp.bfloat16)
        d_value = jnp.einsum("hpt,phd->thd", weight_b.astype(jnp.float32), grad_heads, precision=lax.Precision.HIGHEST).astype(jnp.bfloat16)
        key_nope_grad = d_key[:, :, :NOPE].reshape(key_rows, HEADS * NOPE)
        value_grad = d_value.reshape(key_rows, HEADS * VDIM)
        latent_term = jnp.dot(key_nope_grad, jnp.transpose(key_weight), preferred_element_type=jnp.float32)
        latent_term = latent_term + jnp.dot(value_grad, jnp.transpose(value_weight), preferred_element_type=jnp.float32)
        rope_term = jnp.sum(d_key[:, :, NOPE:].astype(jnp.float32), axis=1)
        partial_grad = jnp.concatenate([latent_term, rope_term], axis=1)
        key_total = totals[0] + jnp.dot(jnp.transpose(latent_rows), key_nope_grad, preferred_element_type=jnp.float32)
        value_total = totals[1] + jnp.dot(jnp.transpose(latent_rows), value_grad, preferred_element_type=jnp.float32)
        return (key_total, value_total), (output.reshape(TOK_DEV, HEADS * VDIM), partial_grad)

    start_totals = (jnp.zeros((LATENT, HEADS * NOPE), jnp.float32), jnp.zeros((LATENT, HEADS * VDIM), jnp.float32))
    totals, emitted = lax.scan(block_step, start_totals, jnp.arange(block_count, dtype=jnp.int32))
    attended = emitted[0].reshape(TOKENS, HEADS * VDIM)
    pieces = emitted[1].reshape(block_count, REACH + 1, TOK_DEV, LATENT + ROPE)
    summed = jnp.zeros((block_count + REACH, TOK_DEV, LATENT + ROPE), jnp.float32)
    for offset in range(REACH + 1):
        summed = summed + jnp.pad(pieces[:, offset], ((offset, REACH - offset), (0, 0), (0, 0)))
    latent_grad = summed[REACH:].reshape(TOKENS, LATENT + ROPE)
    return attended, latent_grad, totals[0], totals[1]
```

```python
import functools
import math

import jax
import jax.numpy as jnp
from jax import lax
from jax.experimental import pallas as pl
from jax.experimental.pallas import tpu as pltpu
from jax.sharding import PartitionSpec as P

NOPE = 128
ROPE = 64
VDIM = 128
LATENT = 512
REACH = 4
PAIR = 2
NEAR = 3
FIN = 2
MESH = pl.DeviceIdType.MESH
F32 = jnp.float32
BF16 = jnp.bfloat16
BACK = REACH // 2
BLOCKS = 2 * (BACK + 1)
QW = PAIR * (NOPE + ROPE)
GW = PAIR * VDIM
WW = PAIR * (NOPE + VDIM)


def dot(a, b, ca, cb):
    return lax.dot_general(a, b, (((ca,), (cb,)), ((), ())), preferred_element_type=F32)


def lag_of(pos):
    return jnp.where(pos > 0, NEAR - 1 + pos, 0)


def kernel(
    n, hn, steps, turns, fin_lag,
    lat_ref, qid_ref, q_ref, g_ref, kw_ref, vw_ref,
    att_ref, lg_ref, kwg_ref, vwg_ref,
    lat_all, lat_t, bias, lgacc, wb, qb, gb, atts, part, rzp, rzm, yr, l1s, l1r, l2s, l2r, lgown, hb,
    w_ls, q_ls, g_ls, q_ss, q_rs, g_ss, g_rs, a_ss, a_rs,
    la_ss, la_rs, lb_ss, lb_rs, lc_ss, lc_rs,
    zp_ss, zm_ss, zp_rs, zm_rs, y_ss, y_rs, l1_ss, l1_rs, l2_ss, l2_rs, h_ss, h_rs,
):
    s = lax.axis_index("seq")
    h = lax.axis_index("head")
    line = n // 2
    z, y = s // 2, s % 2
    other = 1 - y
    mate = s + 1 - 2 * y
    core = h % 2
    twin = h + 1 - 2 * core
    tok = lat_ref.shape[1]
    width = LATENT + ROPE
    keys = BLOCKS * tok
    queries = 2 * tok
    own_heads = steps * PAIR
    to_log2 = 1.0 / math.log(2.0)
    scale = 1.0 / math.sqrt(NOPE + ROPE)

    def remote(src, dst, ss, rs, to):
        return pltpu.make_async_remote_copy(
            src_ref=src, dst_ref=dst, send_sem=ss, recv_sem=rs, device_id=to, device_id_type=MESH
        )

    def cols(half, j, wide):
        return pl.ds(pl.multiple_of(half * (steps * wide) + j * wide, 128), wide)

    def w_copy(j, which):
        ref, col, wide = (kw_ref, 0, PAIR * NOPE) if which == 0 else (vw_ref, PAIR * NOPE, GW)
        return pltpu.make_async_copy(
            ref.at[:, cols(y, j, wide)], wb.at[j, :, pl.ds(col, wide)], w_ls.at[j, which]
        )

    def q_own(j):
        return pltpu.make_async_copy(q_ref.at[:, cols(y, j, QW)], qb.at[j, 0], q_ls.at[j])

    def g_own(j):
        return pltpu.make_async_copy(g_ref.at[:, cols(y, j, GW)], gb.at[j, 0], g_ls.at[j])

    def q_swap(j):
        return remote(q_ref.at[:, cols(other, j, QW)], qb.at[j, 1], q_ss.at[j], q_rs.at[j], (mate, h))

    def g_swap(j):
        return remote(g_ref.at[:, cols(other, j, GW)], gb.at[j, 1], g_ss.at[j], g_rs.at[j], (mate, h))

    def a_swap(j, half):
        return remote(atts.at[j], att_ref.at[:, cols(half, j, GW)], a_ss.at[j], a_rs.at[j], (mate, h))

    def la_copy(k):
        to = mate if k == 0 else s + 2 * k
        return remote(
            lat_all.at[0, core], lat_all.at[1 if k == 0 else 2 * k, core], la_ss.at[k], la_rs.at[k], (to, h)
        )

    def lb_copy(k):
        return remote(
            lat_all.at[2 * k, core], lat_all.at[2 * k + 1, core], lb_ss.at[k - 1], lb_rs.at[k - 1], (mate, h)
        )

    def lc_copy(b, half):
        return remote(lat_all.at[b, half], lat_all.at[b, half], lc_ss.at[b - 1], lc_rs.at[b - 1], (s, twin))

    def z_copy(i, d, up):
        buf, ss, rs = (rzp, zp_ss, zp_rs) if up else (rzm, zm_ss, zm_rs)
        return remote(part.at[i, d], buf.at[i, d], ss.at[i, d], rs.at[i, d], (s + 2 if up else s - 2, h))

    def y_copy(i):
        return remote(part.at[i, z, other], yr.at[i], y_ss.at[i], y_rs.at[i], (mate, h))

    def l1_copy(k):
        return remote(l1s.at[(h + k) % hn], l1r.at[k - 1], l1_ss.at[k - 1], l1_rs.at[k - 1], (s, (h + k) % hn))

    def l2_copy(b):
        base = s if b % 2 == 0 else mate
        return remote(l2s.at[b - 1], l2r.at[b - 1], l2_ss.at[b - 1], l2_rs.at[b - 1], (base - 2 * (b // 2), h))

    def h_copy(k, slot):
        return remote(hb.at[slot], hb.at[slot], h_ss.at[k - 1], h_rs.at[slot], (s, (h + k) % hn))

    def enter():
        w_copy(0, 0).start()
        w_copy(0, 1).start()
        q_own(0).start()
        g_own(0).start()
        barrier = pltpu.get_barrier_semaphore()

        def greet(to):
            pl.semaphore_signal(barrier, inc=1, device_id=to, device_id_type=MESH)

        greet((mate, h))
        for k in range(1, BACK + 1):
            @pl.when(z + k < line)
            def _():
                greet((s + 2 * k, h))
                greet((mate + 2 * k, h))

            @pl.when(z - k >= 0)
            def _():
                greet((s - 2 * k, h))
                greet((mate - 2 * k, h))
        for k in range(1, hn):
            greet((s, (h + k) % hn))
        ids = jnp.transpose(jnp.broadcast_to(qid_ref[...].astype(F32), (tok, tok)))
        mine = jnp.transpose(lat_ref[...].astype(F32))
        packed = jnp.concatenate([mine, ids[:, :lat_all.shape[3] - width]], axis=1).astype(BF16)
        lat_all[0] = packed.reshape(lat_all.shape[1:])
        pl.semaphore_wait(barrier, 2 * (jnp.minimum(z, BACK) + jnp.minimum(line - 1 - z, BACK)) + hn)
        la_copy(0).start()
        for k in range(1, BACK + 1):
            @pl.when(z + k < line)
            def _():
                la_copy(k).start()
        q_swap(0).start()
        g_swap(0).start()

        def fetch(j, c):
            w_copy(j, 0).start()
            w_copy(j, 1).start()
            q_own(j).start()
            g_own(j).start()
            return c

        lax.fori_loop(1, steps, fetch, 0)
        lgacc[...] = jnp.zeros_like(lgacc)

        @pl.when(z == 0)
        def _():
            for i in range(steps):
                rzp[i, 0] = jnp.zeros(rzp.shape[2:], BF16)

        @pl.when(z == line - 1)
        def _():
            for i in range(steps):
                rzm[i, line - 1] = jnp.zeros(rzm.shape[2:], BF16)

        for k in range(1, BACK + 1):
            @pl.when(z - k >= 0)
            def _():
                la_copy(k).wait_recv()
                lb_copy(k).start()
                lc_copy(2 * k, core).start()

            @pl.when(z - k < 0)
            def _():
                for b in (2 * k, 2 * k + 1):
                    lat_all[b] = jnp.zeros(lat_all.shape[1:], BF16)
        la_copy(0).wait_recv()
        lc_copy(1, core).start()
        for k in range(1, BACK + 1):
            @pl.when(z - k >= 0)
            def _():
                lb_copy(k).wait_recv()
                lc_copy(2 * k + 1, core).start()

        def swap(j, c):
            q_swap(j).start()
            g_swap(j).start()
            return c

        lax.fori_loop(1, steps, swap, 0)
        lc_copy(1, 1 - core).wait_recv()
        for k in range(1, BACK + 1):
            @pl.when(z - k >= 0)
            def _():
                lc_copy(2 * k, 1 - core).wait_recv()
                lc_copy(2 * k + 1, 1 - core).wait_recv()
        rows = lat_all[...].reshape(keys, lat_all.shape[3])
        lat_t[...] = jnp.transpose(rows[:, :LATENT])
        mate_ids = jnp.transpose(rows[tok:2 * tok, LATENT:].astype(F32))[ROPE:ROPE + 1, :]
        row = lax.broadcasted_iota(jnp.int32, (tok, tok), 0)
        col = lax.broadcasted_iota(jnp.int32, (tok, tok), 1)
        for b in range(BLOCKS):
            block = (s if b % 2 == 0 else mate) - 2 * (b // 2)
            key_id = rows[b * tok:(b + 1) * tok, width:width + 1].astype(F32)
            for k in range(2):
                query_id = qid_ref[...].astype(F32) if k == 0 else mate_ids
                first = (s if k == 0 else mate) - block
                visible = (row <= col + first * tok) & (block >= 0) & (key_id == query_id)
                bias[b * tok:(b + 1) * tok, k * tok:(k + 1) * tok] = jnp.where(visible, 0.0, -jnp.inf)

    def compute(j):
        w_copy(j, 0).wait()
        w_copy(j, 1).wait()
        q_own(j).wait()
        g_own(j).wait()
        q_swap(j).wait_recv()
        g_swap(j).wait_recv()
        rows = lat_all[...].reshape(keys, lat_all.shape[3])
        lat = rows[:, :LATENT]
        rope = rows[:, LATENT:width]
        w = wb[j]
        q2 = qb[j].reshape(queries, QW)
        g2 = gb[j].reshape(queries, GW)
        kv = dot(lat, w, 1, 0).astype(BF16)
        dks, dvs, rope_sum = [], [], None
        for a in range(PAIR):
            q = q2[:, a * (NOPE + ROPE):(a + 1) * (NOPE + ROPE)]
            g = g2[:, a * VDIM:(a + 1) * VDIM]
            v = kv[:, PAIR * NOPE + a * VDIM:PAIR * NOPE + (a + 1) * VDIM]
            k = jnp.concatenate([kv[:, a * NOPE:(a + 1) * NOPE], rope], axis=1)
            sc = dot(k, q, 1, 1) * (scale * to_log2) + bias[...]
            e = jnp.exp2(sc - jnp.max(sc, axis=0, keepdims=True))
            p = e * (1.0 / jnp.sum(e, axis=0, keepdims=True))
            pb = p.astype(BF16)
            att = jnp.transpose(dot(v, pb, 0, 0)).astype(BF16)
            att_ref[:, pl.ds(pl.multiple_of((y * own_heads + j * PAIR + a) * VDIM, 128), VDIM)] = att[:tok]
            atts[j, :, a * VDIM:(a + 1) * VDIM] = att[tok:]
            dp = dot(v, g, 1, 1)
            delta = jnp.sum(p * dp, axis=0, keepdims=True)
            ds = (p * (dp - delta) * scale).astype(BF16)
            dk = dot(ds, q, 1, 0)
            dvs.append(dot(pb, g, 1, 0).astype(BF16))
            dks.append(dk[:, :NOPE].astype(BF16))
            r = dk[:, NOPE:]
            rope_sum = r if rope_sum is None else rope_sum + r
        dd = jnp.concatenate(dks + dvs, axis=1)
        part[j] = dot(lat_t[...], dd, 1, 0).astype(BF16).reshape(part.shape[1:])
        flat = lgacc.shape[:3]
        lgacc[:, :, :, :LATENT] += dot(dd, w, 1, 1).reshape(*flat, LATENT)
        lgacc[:, :, :, LATENT:] += rope_sum.reshape(*flat, ROPE)
        a_swap(j, y).start()

    def hop(i, pos, up):
        buf = rzp if up else rzm
        for dist in range(line - 1, 0, -1):
            d = z + dist if up else z - dist

            @pl.when((d < line) & (d >= 0))
            def _():
                @pl.when(pos > 0)
                def _():
                    z_copy(i, d, up).wait_recv()
                    part[i, d] = (part[i, d].astype(F32) + buf[i, d].astype(F32)).astype(BF16)
                z_copy(i, d, up).start()

    def finish(i):
        @pl.when(z > 0)
        def _():
            z_copy(i, z, True).wait_recv()

        @pl.when(z < line - 1)
        def _():
            z_copy(i, z, False).wait_recv()

        def total(yy):
            return part[i, z, yy].astype(F32) + rzp[i, z, yy].astype(F32) + rzm[i, z, yy].astype(F32)

        part[i, z, other] = total(other).astype(BF16)
        y_copy(i).start()
        put(i, y, total(y))

    def put(i, half, rows):
        kwg_ref[:, cols(half, i, PAIR * NOPE)] = rows[:, :PAIR * NOPE]
        vwg_ref[:, cols(half, i, GW)] = rows[:, PAIR * NOPE:]

    def close(i):
        y_copy(i).wait_recv()
        put(i, other, yr[i].astype(F32))

    def latent_send():
        for k in range(hn):
            l1s[k] = lgacc[:, k].astype(BF16)
        for k in range(1, hn):
            l1_copy(k).start()

    def latent_pass():
        for k in range(1, hn):
            l1_copy(k).wait_recv()
        for b in range(BLOCKS):
            tot = lgacc[b, h]
            for k in range(1, hn):
                tot = tot + l1r[k - 1, b].astype(F32)
            if b == 0:
                lgown[...] = tot
            else:
                l2s[b - 1] = tot.astype(BF16)
        for b in range(1, BLOCKS):
            @pl.when(z - b // 2 >= 0)
            def _():
                l2_copy(b).start()

    def latent_gather():
        for b in range(1, BLOCKS):
            @pl.when(z + b // 2 < line)
            def _():
                l2_copy(b).wait_recv()
                lgown[...] += l2r[b - 1].astype(F32)
        hb[h] = lgown[...].astype(BF16)
        for k in range(1, hn):
            h_copy(k, h).start()

    def latent_out():
        for k in range(1, hn):
            h_copy(k, (h + k) % hn).wait_recv()
        lg_ref[...] = jnp.transpose(hb[...].astype(F32).reshape(tok, width))

    enter()

    def turn(j, c):
        @pl.when(j < steps)
        def _():
            compute(j)

        @pl.when(j == steps - 1)
        def _():
            latent_send()

        for up in (True, False):
            pos = z if up else line - 1 - z
            i = j - lag_of(pos)

            @pl.when((i >= 0) & (i < steps))
            def _():
                hop(i, pos, up)

        @pl.when(j == steps + 1)
        def _():
            latent_pass()

        @pl.when(j == steps + 2)
        def _():
            latent_gather()

        i = j - fin_lag

        @pl.when((i >= 0) & (i < steps))
        def _():
            finish(i)

        @pl.when((i >= 1) & (i < steps + 1))
        def _():
            close(i - 1)

        return c

    lax.fori_loop(0, turns, turn, 0)
    latent_out()

    def drain(j, c):
        a_swap(j, other).wait_recv()
        a_swap(j, y).wait_send()
        q_swap(j).wait_send()
        g_swap(j).wait_send()
        y_copy(j).wait_send()
        for d in range(line):
            @pl.when(d > z)
            def _():
                z_copy(j, d, True).wait_send()

            @pl.when(d < z)
            def _():
                z_copy(j, d, False).wait_send()
        return c

    lax.fori_loop(0, steps, drain, 0)
    la_copy(0).wait_send()
    lc_copy(1, core).wait_send()
    for k in range(1, BACK + 1):
        @pl.when(z + k < line)
        def _():
            la_copy(k).wait_send()

        @pl.when(z - k >= 0)
        def _():
            lb_copy(k).wait_send()
            lc_copy(2 * k, core).wait_send()
            lc_copy(2 * k + 1, core).wait_send()
    for k in range(1, hn):
        l1_copy(k).wait_send()
        h_copy(k, h).wait_send()
    for b in range(1, BLOCKS):
        @pl.when(z - b // 2 >= 0)
        def _():
            l2_copy(b).wait_send()


def per_device(n, hn, queries, latents, doc_ids, key_weight, value_weight, out_grad):
    tok = latents.shape[0]
    heads = key_weight.shape[1] // NOPE
    steps = heads // 2 // PAIR
    line = n // 2
    rows = LATENT // n
    fin_lag = NEAR + line - 2 + FIN - 1
    turns = steps + max(fin_lag + 1, 3)
    keys = BLOCKS * tok
    width = LATENT + ROPE
    wide = width + 64
    share = tok // hn
    ids = doc_ids.reshape(1, tok)
    whole = pl.BlockSpec(memory_space=pltpu.VMEM)
    far = pl.BlockSpec(memory_space=pltpu.HBM)
    dma = pltpu.SemaphoreType.DMA
    ring = max(hn - 1, 1)
    att, lg, kwg, vwg = pl.pallas_call(
        functools.partial(kernel, n, hn, steps, turns, fin_lag),
        out_shape=(
            pltpu.VMEM((tok, heads * VDIM), BF16),
            pltpu.VMEM((width, tok), F32),
            pltpu.VMEM((rows, heads * NOPE), F32),
            pltpu.VMEM((rows, heads * VDIM), F32),
        ),
        in_specs=[whole, whole, far, far, far, far],
        out_specs=(whole, whole, whole, whole),
        scratch_shapes=[
            pltpu.VMEM((BLOCKS, 2, tok // 2, wide), BF16),
            pltpu.VMEM((LATENT, keys), BF16),
            pltpu.VMEM((keys, 2 * tok), F32),
            pltpu.VMEM((BLOCKS, hn, share, width), F32),
            pltpu.VMEM((steps, LATENT, WW), BF16),
            pltpu.VMEM((steps, 2, tok, QW), BF16),
            pltpu.VMEM((steps, 2, tok, GW), BF16),
            pltpu.VMEM((steps, tok, GW), BF16),
            pltpu.VMEM((steps, line, 2, rows, WW), BF16),
            pltpu.VMEM((steps, line, 2, rows, WW), BF16),
            pltpu.VMEM((steps, line, 2, rows, WW), BF16),
            pltpu.VMEM((steps, rows, WW), BF16),
            pltpu.VMEM((hn, BLOCKS, share, width), BF16),
            pltpu.VMEM((ring, BLOCKS, share, width), BF16),
            pltpu.VMEM((BLOCKS - 1, share, width), BF16),
            pltpu.VMEM((BLOCKS - 1, share, width), BF16),
            pltpu.VMEM((share, width), F32),
            pltpu.VMEM((hn, share, width), BF16),
            dma((steps, 2)), dma((steps,)), dma((steps,)),
            dma((steps,)), dma((steps,)), dma((steps,)), dma((steps,)), dma((steps,)), dma((steps,)),
            dma((BACK + 1,)), dma((BACK + 1,)), dma((BACK,)), dma((BACK,)), dma((BLOCKS - 1,)), dma((BLOCKS - 1,)),
            dma((steps, line)), dma((steps, line)), dma((steps, line)), dma((steps, line)),
            dma((steps,)), dma((steps,)),
            dma((ring,)), dma((ring,)), dma((BLOCKS - 1,)), dma((BLOCKS - 1,)), dma((ring,)), dma((hn,)),
        ],
        compiler_params=pltpu.CompilerParams(
            collective_id=0,
            has_side_effects=True,
            vmem_limit_bytes=48 * 1024 * 1024,
        ),
    )(latents.T, ids, queries, out_grad, key_weight, value_weight)
    return att, lg.T, kwg, vwg


def solution(mesh):
    in_specs = (
        P("seq", "head"),
        P("seq", None),
        P("seq"),
        P(None, "head"),
        P(None, "head"),
        P("seq", "head"),
    )
    out_specs = (P("seq", "head"), P("seq", None), P("seq", "head"), P("seq", "head"))
    body = functools.partial(per_device, mesh.shape["seq"], mesh.shape["head"])
    return jax.shard_map(
        body, mesh=mesh, in_specs=in_specs, out_specs=out_specs, check_vma=False
    )
```

```python
import functools
import math

import jax
import jax.numpy as jnp
from jax import lax
from jax.experimental import pallas as pl
from jax.experimental.pallas import tpu as pltpu
from jax.sharding import PartitionSpec as P

NOPE = 128
ROPE = 64
VDIM = 128
LATENT = 512
REACH = 4
PAIR = 2
NEAR = 3
VMEM_LIMIT = 60 * 1024 * 1024
FIN = 2
MESH = pl.DeviceIdType.MESH
F32 = jnp.float32
BF16 = jnp.bfloat16
BACK = REACH // 2
BLOCKS = 2 * (BACK + 1)
QW = PAIR * (NOPE + ROPE)
GW = PAIR * VDIM
WW = PAIR * (NOPE + VDIM)


def dot(a, b, ca, cb):
    return lax.dot_general(a, b, (((ca,), (cb,)), ((), ())), preferred_element_type=F32)


def lag_of(pos):
    return jnp.where(pos > 0, NEAR - 1 + pos, 0)


def kernel(
    n, hn, steps, turns, fin_lag,
    lat_hbm, qid_hbm, q_ref, g_ref, kw_ref, vw_ref,
    att_ref, lg_ref, kwg_ref, vwg_ref,
    lat_ref, qid_ref, lat_all, lat_t, bias, lgacc, wb, qb, gb, atts, part, rzp, rzm, yr, l1s, l1r, l2s, l2r, lgown, hb,
    in_ls, w_ls, q_ls, g_ls, q_ss, q_rs, g_ss, g_rs, a_ss, a_rs,
    la_ss, la_rs, lb_ss, lb_rs, lc_ss, lc_rs,
    zp_ss, zm_ss, zp_rs, zm_rs, y_ss, y_rs, l1_ss, l1_rs, l2_ss, l2_rs, h_ss, h_rs,
):
    s = lax.axis_index("seq")
    h = lax.axis_index("head")
    line = n // 2
    z, y = s // 2, s % 2
    other = 1 - y
    mate = s + 1 - 2 * y
    core = h % 2
    twin = h + 1 - 2 * core
    tok = lat_ref.shape[1]
    width = LATENT + ROPE
    keys = BLOCKS * tok
    queries = 2 * tok
    own_heads = steps * PAIR
    to_log2 = 1.0 / math.log(2.0)
    scale = 1.0 / math.sqrt(NOPE + ROPE)

    def remote(src, dst, ss, rs, to):
        return pltpu.make_async_remote_copy(
            src_ref=src, dst_ref=dst, send_sem=ss, recv_sem=rs, device_id=to, device_id_type=MESH
        )

    def cols(half, j, wide):
        return pl.ds(pl.multiple_of(half * (steps * wide) + j * wide, 128), wide)

    def w_copy(j, which):
        ref, col, wide = (kw_ref, 0, PAIR * NOPE) if which == 0 else (vw_ref, PAIR * NOPE, GW)
        return pltpu.make_async_copy(
            ref.at[:, cols(y, j, wide)], wb.at[j, :, pl.ds(col, wide)], w_ls.at[j, which]
        )

    def q_own(j):
        return pltpu.make_async_copy(q_ref.at[:, cols(y, j, QW)], qb.at[j, 0], q_ls.at[j])

    def g_own(j):
        return pltpu.make_async_copy(g_ref.at[:, cols(y, j, GW)], gb.at[j, 0], g_ls.at[j])

    def q_swap(j):
        return remote(q_ref.at[:, cols(other, j, QW)], qb.at[j, 1], q_ss.at[j], q_rs.at[j], (mate, h))

    def g_swap(j):
        return remote(g_ref.at[:, cols(other, j, GW)], gb.at[j, 1], g_ss.at[j], g_rs.at[j], (mate, h))

    def a_swap(j, half):
        return remote(atts.at[j], att_ref.at[:, cols(half, j, GW)], a_ss.at[j], a_rs.at[j], (mate, h))

    def la_copy(k):
        to = mate if k == 0 else s + 2 * k
        return remote(
            lat_all.at[0, core], lat_all.at[1 if k == 0 else 2 * k, core], la_ss.at[k], la_rs.at[k], (to, h)
        )

    def lb_copy(k):
        return remote(
            lat_all.at[2 * k, core], lat_all.at[2 * k + 1, core], lb_ss.at[k - 1], lb_rs.at[k - 1], (mate, h)
        )

    def lc_copy(b, half):
        return remote(lat_all.at[b, half], lat_all.at[b, half], lc_ss.at[b - 1], lc_rs.at[b - 1], (s, twin))

    def z_copy(i, d, up):
        buf, ss, rs = (rzp, zp_ss, zp_rs) if up else (rzm, zm_ss, zm_rs)
        return remote(part.at[i, d], buf.at[i, d], ss.at[i, d], rs.at[i, d], (s + 2 if up else s - 2, h))

    def y_copy(i):
        return remote(part.at[i, z, other], yr.at[i], y_ss.at[i], y_rs.at[i], (mate, h))

    def l1_copy(k):
        return remote(l1s.at[(h + k) % hn], l1r.at[k - 1], l1_ss.at[k - 1], l1_rs.at[k - 1], (s, (h + k) % hn))

    def l2_copy(b):
        base = s if b % 2 == 0 else mate
        return remote(l2s.at[b - 1], l2r.at[b - 1], l2_ss.at[b - 1], l2_rs.at[b - 1], (base - 2 * (b // 2), h))

    def h_copy(k, slot):
        return remote(hb.at[slot], hb.at[slot], h_ss.at[k - 1], h_rs.at[slot], (s, (h + k) % hn))

    def enter():
        loads = [
            pltpu.make_async_copy(src, dst, in_ls.at[k])
            for k, (src, dst) in enumerate(((lat_hbm, lat_ref), (qid_hbm, qid_ref)))
        ]
        for load in loads:
            load.start()
        w_copy(0, 0).start()
        w_copy(0, 1).start()
        q_own(0).start()
        g_own(0).start()
        barrier = pltpu.get_barrier_semaphore()

        def greet(to):
            pl.semaphore_signal(barrier, inc=1, device_id=to, device_id_type=MESH)

        greet((mate, h))
        for k in range(1, BACK + 1):
            @pl.when(z + k < line)
            def _():
                greet((s + 2 * k, h))
                greet((mate + 2 * k, h))

            @pl.when(z - k >= 0)
            def _():
                greet((s - 2 * k, h))
                greet((mate - 2 * k, h))
        for k in range(1, hn):
            greet((s, (h + k) % hn))
        for load in loads:
            load.wait()
        ids = jnp.transpose(jnp.broadcast_to(qid_ref[...].astype(F32), (tok, tok)))
        mine = jnp.transpose(lat_ref[...].astype(F32))
        packed = jnp.concatenate([mine, ids[:, :lat_all.shape[3] - width]], axis=1).astype(BF16)
        lat_all[0] = packed.reshape(lat_all.shape[1:])
        pl.semaphore_wait(barrier, 2 * (jnp.minimum(z, BACK) + jnp.minimum(line - 1 - z, BACK)) + hn)
        la_copy(0).start()
        for k in range(1, BACK + 1):
            @pl.when(z + k < line)
            def _():
                la_copy(k).start()
        q_swap(0).start()
        g_swap(0).start()

        def fetch(j, c):
            w_copy(j, 0).start()
            w_copy(j, 1).start()
            q_own(j).start()
            g_own(j).start()
            return c

        lax.fori_loop(1, steps, fetch, 0)
        lgacc[...] = jnp.zeros_like(lgacc)

        @pl.when(z == 0)
        def _():
            for i in range(steps):
                rzp[i, 0] = jnp.zeros(rzp.shape[2:], BF16)

        @pl.when(z == line - 1)
        def _():
            for i in range(steps):
                rzm[i, line - 1] = jnp.zeros(rzm.shape[2:], BF16)

        for k in range(1, BACK + 1):
            @pl.when(z - k >= 0)
            def _():
                la_copy(k).wait_recv()
                lb_copy(k).start()
                lc_copy(2 * k, core).start()

            @pl.when(z - k < 0)
            def _():
                for b in (2 * k, 2 * k + 1):
                    lat_all[b] = jnp.zeros(lat_all.shape[1:], BF16)
        la_copy(0).wait_recv()
        lc_copy(1, core).start()
        for k in range(1, BACK + 1):
            @pl.when(z - k >= 0)
            def _():
                lb_copy(k).wait_recv()
                lc_copy(2 * k + 1, core).start()

        def swap(j, c):
            q_swap(j).start()
            g_swap(j).start()
            return c

        lax.fori_loop(1, steps, swap, 0)
        lc_copy(1, 1 - core).wait_recv()
        for k in range(1, BACK + 1):
            @pl.when(z - k >= 0)
            def _():
                lc_copy(2 * k, 1 - core).wait_recv()
                lc_copy(2 * k + 1, 1 - core).wait_recv()
        rows = lat_all[...].reshape(keys, lat_all.shape[3])
        lat_t[...] = jnp.transpose(rows[:, :LATENT])
        mate_ids = jnp.transpose(rows[tok:2 * tok, LATENT:].astype(F32))[ROPE:ROPE + 1, :]
        row = lax.broadcasted_iota(jnp.int32, (tok, tok), 0)
        col = lax.broadcasted_iota(jnp.int32, (tok, tok), 1)
        for b in range(BLOCKS):
            block = (s if b % 2 == 0 else mate) - 2 * (b // 2)
            key_id = rows[b * tok:(b + 1) * tok, width:width + 1].astype(F32)
            for k in range(2):
                query_id = qid_ref[...].astype(F32) if k == 0 else mate_ids
                first = (s if k == 0 else mate) - block
                visible = (row <= col + first * tok) & (block >= 0) & (key_id == query_id)
                bias[b * tok:(b + 1) * tok, k * tok:(k + 1) * tok] = jnp.where(visible, 0.0, -jnp.inf)

    def compute(j):
        w_copy(j, 0).wait()
        w_copy(j, 1).wait()
        q_own(j).wait()
        g_own(j).wait()
        q_swap(j).wait_recv()
        g_swap(j).wait_recv()
        rows = lat_all[...].reshape(keys, lat_all.shape[3])
        lat = rows[:, :LATENT]
        rope = rows[:, LATENT:width]
        w = wb[j]
        q2 = qb[j].reshape(queries, QW)
        g2 = gb[j].reshape(queries, GW)
        kv = dot(lat, w, 1, 0).astype(BF16)
        dks, dvs, rope_sum = [], [], None
        for a in range(PAIR):
            q = q2[:, a * (NOPE + ROPE):(a + 1) * (NOPE + ROPE)]
            g = g2[:, a * VDIM:(a + 1) * VDIM]
            v = kv[:, PAIR * NOPE + a * VDIM:PAIR * NOPE + (a + 1) * VDIM]
            k = jnp.concatenate([kv[:, a * NOPE:(a + 1) * NOPE], rope], axis=1)
            sc = dot(k, q, 1, 1) * (scale * to_log2) + bias[...]
            e = jnp.exp2(sc - jnp.max(sc, axis=0, keepdims=True))
            p = e * (1.0 / jnp.sum(e, axis=0, keepdims=True))
            pb = p.astype(BF16)
            att = jnp.transpose(dot(v, pb, 0, 0)).astype(BF16)
            att_ref[:, pl.ds(pl.multiple_of((y * own_heads + j * PAIR + a) * VDIM, 128), VDIM)] = att[:tok]
            atts[j, :, a * VDIM:(a + 1) * VDIM] = att[tok:]
            dp = dot(v, g, 1, 1)
            delta = jnp.sum(p * dp, axis=0, keepdims=True)
            ds = (p * (dp - delta) * scale).astype(BF16)
            dk = dot(ds, q, 1, 0)
            dvs.append(dot(pb, g, 1, 0).astype(BF16))
            dks.append(dk[:, :NOPE].astype(BF16))
            r = dk[:, NOPE:]
            rope_sum = r if rope_sum is None else rope_sum + r
        dd = jnp.concatenate(dks + dvs, axis=1)
        part[j] = dot(lat_t[...], dd, 1, 0).astype(BF16).reshape(part.shape[1:])
        flat = lgacc.shape[:3]
        lgacc[:, :, :, :LATENT] += dot(dd, w, 1, 1).reshape(*flat, LATENT)
        lgacc[:, :, :, LATENT:] += rope_sum.reshape(*flat, ROPE)
        a_swap(j, y).start()

    def hop(i, pos, up):
        buf = rzp if up else rzm
        for dist in range(line - 1, 0, -1):
            d = z + dist if up else z - dist

            @pl.when((d < line) & (d >= 0))
            def _():
                @pl.when(pos > 0)
                def _():
                    z_copy(i, d, up).wait_recv()
                    part[i, d] = (part[i, d].astype(F32) + buf[i, d].astype(F32)).astype(BF16)
                z_copy(i, d, up).start()

    def finish(i):
        @pl.when(z > 0)
        def _():
            z_copy(i, z, True).wait_recv()

        @pl.when(z < line - 1)
        def _():
            z_copy(i, z, False).wait_recv()

        def total(yy):
            return part[i, z, yy].astype(F32) + rzp[i, z, yy].astype(F32) + rzm[i, z, yy].astype(F32)

        part[i, z, other] = total(other).astype(BF16)
        y_copy(i).start()
        put(i, y, total(y))

    def put(i, half, rows):
        kwg_ref[:, cols(half, i, PAIR * NOPE)] = rows[:, :PAIR * NOPE]
        vwg_ref[:, cols(half, i, GW)] = rows[:, PAIR * NOPE:]

    def close(i):
        y_copy(i).wait_recv()
        put(i, other, yr[i].astype(F32))

    def latent_send():
        for k in range(hn):
            l1s[k] = lgacc[:, k].astype(BF16)
        for k in range(1, hn):
            l1_copy(k).start()

    def latent_pass():
        for k in range(1, hn):
            l1_copy(k).wait_recv()
        for b in range(BLOCKS):
            tot = lgacc[b, h]
            for k in range(1, hn):
                tot = tot + l1r[k - 1, b].astype(F32)
            if b == 0:
                lgown[...] = tot
            else:
                l2s[b - 1] = tot.astype(BF16)
        for b in range(1, BLOCKS):
            @pl.when(z - b // 2 >= 0)
            def _():
                l2_copy(b).start()

    def latent_gather():
        for b in range(1, BLOCKS):
            @pl.when(z + b // 2 < line)
            def _():
                l2_copy(b).wait_recv()
                lgown[...] += l2r[b - 1].astype(F32)
        hb[h] = lgown[...].astype(BF16)
        for k in range(1, hn):
            h_copy(k, h).start()

    def latent_out():
        for k in range(1, hn):
            h_copy(k, (h + k) % hn).wait_recv()
        lg_ref[...] = jnp.transpose(hb[...].astype(F32).reshape(tok, width))

    enter()

    def turn(j, c):
        @pl.when(j < steps)
        def _():
            compute(j)

        @pl.when(j == steps - 1)
        def _():
            latent_send()

        for up in (True, False):
            pos = z if up else line - 1 - z
            i = j - lag_of(pos)

            @pl.when((i >= 0) & (i < steps))
            def _():
                hop(i, pos, up)

        @pl.when(j == steps + 1)
        def _():
            latent_pass()

        @pl.when(j == steps + 2)
        def _():
            latent_gather()

        i = j - fin_lag

        @pl.when((i >= 0) & (i < steps))
        def _():
            finish(i)

        @pl.when((i >= 1) & (i < steps + 1))
        def _():
            close(i - 1)

        return c

    lax.fori_loop(0, turns, turn, 0)
    latent_out()

    def drain(j, c):
        a_swap(j, other).wait_recv()
        a_swap(j, y).wait_send()
        q_swap(j).wait_send()
        g_swap(j).wait_send()
        y_copy(j).wait_send()
        for d in range(line):
            @pl.when(d > z)
            def _():
                z_copy(j, d, True).wait_send()

            @pl.when(d < z)
            def _():
                z_copy(j, d, False).wait_send()
        return c

    lax.fori_loop(0, steps, drain, 0)
    la_copy(0).wait_send()
    lc_copy(1, core).wait_send()
    for k in range(1, BACK + 1):
        @pl.when(z + k < line)
        def _():
            la_copy(k).wait_send()

        @pl.when(z - k >= 0)
        def _():
            lb_copy(k).wait_send()
            lc_copy(2 * k, core).wait_send()
            lc_copy(2 * k + 1, core).wait_send()
    for k in range(1, hn):
        l1_copy(k).wait_send()
        h_copy(k, h).wait_send()
    for b in range(1, BLOCKS):
        @pl.when(z - b // 2 >= 0)
        def _():
            l2_copy(b).wait_send()


def flush(*refs):
    sems = refs[-1]
    copies = [pltpu.make_async_copy(refs[k], refs[4 + k], sems.at[k]) for k in range(4)]
    for copy in copies:
        copy.start()
    for copy in copies:
        copy.wait()


def per_device(n, hn, queries, latents, doc_ids, key_weight, value_weight, out_grad):
    tok = latents.shape[0]
    heads = key_weight.shape[1] // NOPE
    steps = heads // 2 // PAIR
    line = n // 2
    rows = LATENT // n
    fin_lag = NEAR + line - 2 + FIN - 1
    turns = steps + max(fin_lag + 1, 3)
    keys = BLOCKS * tok
    width = LATENT + ROPE
    wide = width + 64
    share = tok // hn
    ids = doc_ids.reshape(1, tok)
    whole = pl.BlockSpec(memory_space=pltpu.VMEM)
    far = pl.BlockSpec(memory_space=pltpu.HBM)
    dma = pltpu.SemaphoreType.DMA
    ring = max(hn - 1, 1)
    att, lg, kwg, vwg = pl.pallas_call(
        functools.partial(kernel, n, hn, steps, turns, fin_lag),
        out_shape=(
            pltpu.VMEM((tok, heads * VDIM), BF16),
            pltpu.VMEM((width, tok), F32),
            pltpu.VMEM((rows, heads * NOPE), F32),
            pltpu.VMEM((rows, heads * VDIM), F32),
        ),
        in_specs=[far] * 6,
        out_specs=(whole, whole, whole, whole),
        scratch_shapes=[
            pltpu.VMEM((width, tok), BF16),
            pltpu.VMEM((1, tok), jnp.int32),
            pltpu.VMEM((BLOCKS, 2, tok // 2, wide), BF16),
            pltpu.VMEM((LATENT, keys), BF16),
            pltpu.VMEM((keys, 2 * tok), F32),
            pltpu.VMEM((BLOCKS, hn, share, width), F32),
            pltpu.VMEM((steps, LATENT, WW), BF16),
            pltpu.VMEM((steps, 2, tok, QW), BF16),
            pltpu.VMEM((steps, 2, tok, GW), BF16),
            pltpu.VMEM((steps, tok, GW), BF16),
            pltpu.VMEM((steps, line, 2, rows, WW), BF16),
            pltpu.VMEM((steps, line, 2, rows, WW), BF16),
            pltpu.VMEM((steps, line, 2, rows, WW), BF16),
            pltpu.VMEM((steps, rows, WW), BF16),
            pltpu.VMEM((hn, BLOCKS, share, width), BF16),
            pltpu.VMEM((ring, BLOCKS, share, width), BF16),
            pltpu.VMEM((BLOCKS - 1, share, width), BF16),
            pltpu.VMEM((BLOCKS - 1, share, width), BF16),
            pltpu.VMEM((share, width), F32),
            pltpu.VMEM((hn, share, width), BF16),
            dma((2,)), dma((steps, 2)), dma((steps,)), dma((steps,)),
            dma((steps,)), dma((steps,)), dma((steps,)), dma((steps,)), dma((steps,)), dma((steps,)),
            dma((BACK + 1,)), dma((BACK + 1,)), dma((BACK,)), dma((BACK,)), dma((BLOCKS - 1,)), dma((BLOCKS - 1,)),
            dma((steps, line)), dma((steps, line)), dma((steps, line)), dma((steps, line)),
            dma((steps,)), dma((steps,)),
            dma((ring,)), dma((ring,)), dma((BLOCKS - 1,)), dma((BLOCKS - 1,)), dma((ring,)), dma((hn,)),
        ],
        compiler_params=pltpu.CompilerParams(
            collective_id=0,
            has_side_effects=True,
            vmem_limit_bytes=VMEM_LIMIT,
        ),
    )(latents.T, ids, queries, out_grad, key_weight, value_weight)
    out = (att, lg, kwg, vwg)
    att, lg, kwg, vwg = pl.pallas_call(
        flush,
        out_shape=tuple(pltpu.HBM(o.shape, o.dtype) for o in out),
        in_specs=[whole] * 4,
        out_specs=(far,) * 4,
        scratch_shapes=[dma((4,))],
        compiler_params=pltpu.CompilerParams(vmem_limit_bytes=1024 * 1024),
    )(*out)
    return att, lg.T, kwg, vwg


def solution(mesh):
    in_specs = (
        P("seq", "head"),
        P("seq", None),
        P("seq"),
        P(None, "head"),
        P(None, "head"),
        P("seq", "head"),
    )
    out_specs = (P("seq", "head"), P("seq", None), P("seq", "head"), P("seq", "head"))
    body = functools.partial(per_device, mesh.shape["seq"], mesh.shape["head"])
    return jax.shard_map(
        body, mesh=mesh, in_specs=in_specs, out_specs=out_specs, check_vma=False
    )
```

```python
import functools
import math

import jax
import jax.numpy as jnp
from jax import lax
from jax.experimental import pallas as pl
from jax.experimental.pallas import tpu as pltpu
from jax.sharding import PartitionSpec as P

NOPE = 128
ROPE = 64
VDIM = 128
LATENT = 512
REACH = 4
PAIR = 2
LEND = 3
LATE = 2
VMEM_LIMIT = 60 * 1024 * 1024
MESH = pl.DeviceIdType.MESH
F32 = jnp.float32
BF16 = jnp.bfloat16
BACK = REACH // 2
BLOCKS = 2 * (BACK + 1)
SPAN = BLOCKS + 2
QW = PAIR * (NOPE + ROPE)
GW = PAIR * VDIM
WW = PAIR * (NOPE + VDIM)


def dot(a, b, ca, cb):
    return lax.dot_general(a, b, (((ca,), (cb,)), ((), ())), preferred_element_type=F32)


def pick(table, t):
    out = jnp.int32(0)
    for k, v in enumerate(table):
        if v:
            out = out + jnp.where(t == k, v, 0)
    return out


def plan(chunks, line):
    lent = max(1, chunks * LEND // 8)
    plain = chunks - lent
    late = min(LATE, plain)
    order = [("L", c) for c in range(max(1, lent - 1))] + [("N", lent)]
    order += [("L", c) for c in range(max(1, lent - 1), lent)] + [("N", c) for c in range(lent + 1, chunks)]
    turns, ready, own = [], {}, {}
    for kind, c in order:
        own[c] = len(turns)
        turns.append((c, 0))
        if kind == "L":
            turns.append((c, 1))
        ready[c] = len(turns) - 1
    work = len(turns)
    tail = work - 1 + max(late * (line - 2), 2 * (line - 3) + late - 1) + 1
    done = {}
    for c in range(chunks):
        late_rank = c - (chunks - late)
        done[c] = ready[c] + 2 * (line - 2) if late_rank < 0 else tail + late_rank
    return lent, plain, late, turns, ready, [c for _, c in order], done


def kernel(
    n, hn, chunks,
    lat_hbm, qid_hbm, q_ref, g_ref, kw_ref, vw_ref,
    att_ref, lg_ref, kwg_ref, vwg_ref,
    lat_ref, qid_ref, lat_all, lat_t, bias, lgacc, wb, qb, gb, atts, part, rzp, rzm, yr,
    l1s, l1r, twos, xs, xr, l2s, l2r, lgown, hb,
    in_ls, w_ls, q_ls, g_ls, q_ss, q_rs, g_ss, g_rs, qe_ss, qe_rs, ge_ss, ge_rs, a_ss, a_rs, ae_rs,
    la_ss, la_rs, lb_ss, lb_rs, lc_ss, lc_rs,
    zp_ss, zm_ss, zp_rs, zm_rs, y_ss, y_rs, l1_ss, l1_rs, x_ss, x_rs, l2_ss, l2_rs, h_ss, h_rs,
):
    s = lax.axis_index("seq")
    h = lax.axis_index("head")
    line = n // 2
    lent, plain, late, turns, ready, order, done = plan(chunks, line)
    work = len(turns)
    z, y = s // 2, s % 2
    other = 1 - y
    mate = s + 1 - 2 * y
    core = h % 2
    twin = h + 1 - 2 * core
    chips = hn // 2
    chip = h // 2
    tok = lat_ref.shape[1]
    width = LATENT + ROPE
    keys = BLOCKS * tok
    queries = 2 * tok
    to_log2 = 1.0 / math.log(2.0)
    scale = 1.0 / math.sqrt(NOPE + ROPE)
    low, high = z == 0, z == line - 1
    edge = low | high
    inner = jnp.logical_not(edge)
    borrows_low, borrows_high = z == 1, z == line - 2
    borrows = borrows_low | borrows_high
    step = jnp.where(low | borrows_high, 2, -2)

    def remote(src, dst, ss, rs, to):
        return pltpu.make_async_remote_copy(
            src_ref=src, dst_ref=dst, send_sem=ss, recv_sem=rs, device_id=to, device_id_type=MESH
        )

    def cols(half, j, wide):
        return pl.ds(pl.multiple_of(half * (chunks * wide) + j * wide, 128), wide)

    def w_copy(j, which):
        ref, col, wide = (kw_ref, 0, PAIR * NOPE) if which == 0 else (vw_ref, PAIR * NOPE, GW)
        return pltpu.make_async_copy(
            ref.at[:, cols(y, j, wide)], wb.at[j, :, pl.ds(col, wide)], w_ls.at[j, which]
        )

    def q_own(j):
        return pltpu.make_async_copy(q_ref.at[:, cols(y, j, QW)], qb.at[j, 0], q_ls.at[j])

    def g_own(j):
        return pltpu.make_async_copy(g_ref.at[:, cols(y, j, GW)], gb.at[j, 0], g_ls.at[j])

    def q_swap(j):
        return remote(q_ref.at[:, cols(other, j, QW)], qb.at[j, 1], q_ss.at[j], q_rs.at[j], (mate, h))

    def g_swap(j):
        return remote(g_ref.at[:, cols(other, j, GW)], gb.at[j, 1], g_ss.at[j], g_rs.at[j], (mate, h))

    def q_lend(c, k):
        src = q_ref.at[:, cols(y, c, QW)] if k == 0 else qb.at[c, 1]
        return remote(src, qb.at[chunks + c, k], qe_ss.at[c, k], qe_rs.at[c, k], (s + step, h))

    def g_lend(c, k):
        src = g_ref.at[:, cols(y, c, GW)] if k == 0 else gb.at[c, 1]
        return remote(src, gb.at[chunks + c, k], ge_ss.at[c, k], ge_rs.at[c, k], (s + step, h))

    def a_swap(j, half):
        return remote(atts.at[j, 1], att_ref.at[:, cols(half, j, GW)], a_ss.at[j, 1], a_rs.at[j], (mate, h))

    def a_lent(c, k):
        return remote(atts.at[chunks + c, k], atts.at[c, k], a_ss.at[chunks + c, k], ae_rs.at[c, k], (s + step, h))

    def la_copy(k):
        to, b = (mate, 3) if k == 0 else (s + 2 * k, 2 * (k + 1))
        return remote(lat_all.at[2, core], lat_all.at[b, core], la_ss.at[k + 1], la_rs.at[k + 1], (to, h))

    def lb_copy(k):
        b = 2 * (k + 1)
        return remote(lat_all.at[b, core], lat_all.at[b + 1, core], lb_ss.at[k + 1], lb_rs.at[k + 1], (mate, h))

    def lc_copy(b, half):
        return remote(lat_all.at[b, half], lat_all.at[b, half], lc_ss.at[b], lc_rs.at[b], (s, twin))

    def sends_to(k):
        return high if k < 0 else z + k < line

    def gets_from(k):
        return borrows_high if k < 0 else z - k >= 0

    PAIRS = [p for p in range(SPAN // 2 - 1, -1, -1) if p != 1] + [1]
    FAR = [k for k in range(-1, BACK + 1) if k != 0]

    def z_copy(i, d, up):
        buf, ss, rs = (rzp, zp_ss, zp_rs) if up else (rzm, zm_ss, zm_rs)
        return remote(part.at[i, d], buf.at[i, d], ss.at[i, d], rs.at[i, d], (s + 2 if up else s - 2, h))

    def y_copy(i):
        return remote(part.at[i, z, other], yr.at[i], y_ss.at[i], y_rs.at[i], (mate, h))

    def l1_copy():
        return remote(l1s, l1r, l1_ss.at[0], l1_rs.at[0], (s, twin))

    def x_copy(k, p):
        at = pl.ds(2 * p, 2)
        return remote(
            xs.at[k - 1, at], xr.at[k - 1, at], x_ss.at[k - 1, p], x_rs.at[k - 1, p], (s, (h + 2 * k) % hn)
        )

    def l2_copy(b):
        base = s if b % 2 == 0 else mate
        return remote(l2s.at[b], l2r.at[b], l2_ss.at[b], l2_rs.at[b], (base - 2 * (b // 2 - 1), h))

    def h_copy(k, slot):
        return remote(hb.at[slot], hb.at[slot], h_ss.at[k - 1], h_rs.at[slot], (s, (h + k) % hn))

    def lend_mate(c):
        q_swap(c).wait_recv()
        g_swap(c).wait_recv()
        q_lend(c, 1).start()
        g_lend(c, 1).start()

    def enter():
        loads = [
            pltpu.make_async_copy(src, dst, in_ls.at[k])
            for k, (src, dst) in enumerate(((lat_hbm, lat_ref), (qid_hbm, qid_ref)))
        ]
        for load in loads:
            load.start()
        barrier = pltpu.get_barrier_semaphore()

        def greet(to):
            pl.semaphore_signal(barrier, inc=1, device_id=to, device_id_type=MESH)

        greet((mate, h))
        for k in range(1, BACK + 1):
            @pl.when(z + k < line)
            def _():
                greet((s + 2 * k, h))
                greet((mate + 2 * k, h))

            @pl.when(z - k >= 0)
            def _():
                greet((s - 2 * k, h))
                greet((mate - 2 * k, h))
        for k in range(1, hn):
            greet((s, (h + k) % hn))
        for load in loads:
            load.wait()
        ids = jnp.transpose(jnp.broadcast_to(qid_ref[...].astype(F32), (tok, tok)))
        mine = jnp.transpose(lat_ref[...].astype(F32))
        packed = jnp.concatenate([mine, ids[:, :lat_all.shape[3] - width]], axis=1).astype(BF16)
        lat_all[2] = packed.reshape(lat_all.shape[1:])
        pl.semaphore_wait(barrier, 2 * (jnp.minimum(z, BACK) + jnp.minimum(line - 1 - z, BACK)) + hn)
        la_copy(0).start()
        for k in FAR:
            @pl.when(sends_to(k))
            def _():
                la_copy(k).start()

        def fetch(c):
            w_copy(c, 0).start()
            w_copy(c, 1).start()
            q_own(c).start()
            g_own(c).start()

        def swap(c):
            q_swap(c).start()
            g_swap(c).start()

        @pl.when(edge)
        def _():
            swap(0)
            for c in range(lent):
                q_lend(c, 0).start()
                g_lend(c, 0).start()
            for c in range(lent, chunks):
                fetch(c)

        @pl.when(inner)
        def _():
            for c in order:
                fetch(c)
            swap(order[0])

        lgacc[...] = jnp.zeros_like(lgacc)
        zero = jnp.zeros(part.shape[1:], BF16)

        def clear(i, c):
            part[i] = zero
            return c

        lax.fori_loop(0, chunks, clear, 0)
        for cond, buf, d, count in (
            (low, rzp, 0, chunks), (borrows_low, rzp, 1, lent),
            (high, rzm, line - 1, chunks), (borrows_high, rzm, line - 2, lent),
        ):
            @pl.when(cond)
            def _():
                for i in range(count):
                    buf[i, d] = jnp.zeros(buf.shape[2:], BF16)

        for k in FAR:
            @pl.when(gets_from(k))
            def _():
                la_copy(k).wait_recv()
                lb_copy(k).start()
                lc_copy(2 * (k + 1), core).start()

            @pl.when(jnp.logical_not(gets_from(k)))
            def _():
                for b in (2 * (k + 1), 2 * (k + 1) + 1):
                    lat_all[b] = jnp.zeros(lat_all.shape[1:], BF16)
        la_copy(0).wait_recv()
        lc_copy(3, core).start()
        for k in FAR:
            @pl.when(gets_from(k))
            def _():
                lb_copy(k).wait_recv()
                lc_copy(2 * (k + 1) + 1, core).start()

        @pl.when(edge)
        def _():
            for c in range(max(lent, plain)):
                if c < plain:
                    swap(lent + c)
                if c + 1 < lent:
                    swap(c + 1)
            lend_mate(0)

        @pl.when(inner)
        def _():
            for c in order[1:]:
                swap(c)

        lc_copy(3, 1 - core).wait_recv()
        for k in FAR:
            @pl.when(gets_from(k))
            def _():
                lc_copy(2 * (k + 1), 1 - core).wait_recv()
                lc_copy(2 * (k + 1) + 1, 1 - core).wait_recv()
        for b in range(SPAN):
            rows = lat_all[b].reshape(tok, lat_all.shape[3])
            lat_t[:, b * tok:(b + 1) * tok] = jnp.transpose(rows[:, :LATENT])

        def ids_of(b):
            tail = lat_all[b].reshape(tok, lat_all.shape[3])[:, LATENT:].astype(F32)
            return jnp.transpose(tail)[ROPE:ROPE + 1, :]

        row = lax.broadcasted_iota(jnp.int32, (tok, tok), 0)
        col = lax.broadcasted_iota(jnp.int32, (tok, tok), 1)

        def mask(which, window, query_at, shift):
            for k in range(2):
                query_id = ids_of(query_at + k)
                for b in range(BLOCKS):
                    back = window // 2 - 1 + b // 2
                    block = (s if b % 2 == 0 else mate) - 2 * back
                    rows = lat_all[window + b].reshape(tok, lat_all.shape[3])
                    key_id = rows[:, width:width + 1].astype(F32)
                    first = (s if k == 0 else mate) + shift - block
                    visible = (row <= col + first * tok) & (block >= 0) & (key_id == query_id)
                    bias[which, b * tok:(b + 1) * tok, k * tok:(k + 1) * tok] = jnp.where(visible, 0.0, -jnp.inf)

        mask(0, 2, 2, 0)

        @pl.when(borrows_low)
        def _():
            mask(1, 2, 4, -2)

        @pl.when(borrows_high)
        def _():
            mask(1, 0, 0, 2)

    def compute(c, is_lent):
        slot = jnp.where(is_lent, chunks + c, c)
        which = jnp.where(is_lent, 1, 0)
        window = jnp.where(is_lent & borrows_high, 0, 2)

        @pl.when(jnp.logical_not(is_lent))
        def _():
            w_copy(c, 0).wait()
            w_copy(c, 1).wait()
            q_own(c).wait()
            g_own(c).wait()
            q_swap(c).wait_recv()
            g_swap(c).wait_recv()

        @pl.when(is_lent)
        def _():
            for k in range(2):
                q_lend(c, k).wait_recv()
                g_lend(c, k).wait_recv()

        rows = lat_all[pl.ds(window, BLOCKS)].reshape(keys, lat_all.shape[3])
        lat = rows[:, :LATENT]
        rope = rows[:, LATENT:width]
        w = wb[c]
        q2 = qb[slot].reshape(queries, QW)
        g2 = gb[slot].reshape(queries, GW)
        kv = dot(lat, w, 1, 0).astype(BF16)
        dks, dvs, rope_sum = [], [], None
        for a in range(PAIR):
            q = q2[:, a * (NOPE + ROPE):(a + 1) * (NOPE + ROPE)]
            g = g2[:, a * VDIM:(a + 1) * VDIM]
            v = kv[:, PAIR * NOPE + a * VDIM:PAIR * NOPE + (a + 1) * VDIM]
            k = jnp.concatenate([kv[:, a * NOPE:(a + 1) * NOPE], rope], axis=1)
            sc = dot(k, q, 1, 1) * (scale * to_log2) + bias[which]
            e = jnp.exp2(sc - jnp.max(sc, axis=0, keepdims=True))
            p = e * (1.0 / jnp.sum(e, axis=0, keepdims=True))
            pb = p.astype(BF16)
            att = jnp.transpose(dot(v, pb, 0, 0)).astype(BF16)
            for k in range(2):
                atts[slot, k, :, a * VDIM:(a + 1) * VDIM] = att[k * tok:(k + 1) * tok]
            dp = dot(v, g, 1, 1)
            delta = jnp.sum(p * dp, axis=0, keepdims=True)
            ds = (p * (dp - delta) * scale).astype(BF16)
            dk = dot(ds, q, 1, 0)
            dvs.append(dot(pb, g, 1, 0).astype(BF16))
            dks.append(dk[:, :NOPE].astype(BF16))
            r = dk[:, NOPE:]
            rope_sum = r if rope_sum is None else rope_sum + r
        dd = jnp.concatenate(dks + dvs, axis=1)
        lat_cols = lat_t[:, pl.ds(pl.multiple_of(window * tok, 128), keys)]
        grad = dot(lat_cols, dd, 1, 0).reshape(part.shape[1:])
        part[c] = (part[c].astype(F32) + grad).astype(BF16)
        flat = (BLOCKS,) + lgacc.shape[1:4]
        at = pl.ds(window, BLOCKS)
        lgacc[at, :, :, :, :LATENT] += dot(dd, w, 1, 1).reshape(*flat, LATENT)
        lgacc[at, :, :, :, LATENT:] += rope_sum.reshape(*flat, ROPE)

        @pl.when(is_lent)
        def _():
            for k in range(2):
                a_lent(c, k).start()

        @pl.when(jnp.logical_not(is_lent))
        def _():
            a_swap(c, y).start()
            att_ref[:, cols(y, c, GW)] = atts[c, 0]

    def pass_on(i, r, up, first):
        d = line - 1 - r if up else r

        @pl.when(jnp.logical_not(first))
        def _():
            z_copy(i, d, up).wait_recv()
            buf = rzp if up else rzm
            part[i, d] = (part[i, d].astype(F32) + buf[i, d].astype(F32)).astype(BF16)

        z_copy(i, d, up).start()

    def pass_range(i, r0, r1, up, first):
        def one(r, c):
            pass_on(i, r, up, first)
            return c

        lax.fori_loop(r0, r1, one, 0)

    def pass_late(k0, k1, up):
        def one(k, c):
            pass_on(chunks - late + k % late, k // late, up, True)
            return c

        lax.fori_loop(k0, k1, one, 0)

    def relay(j, up):
        pos = z if up else line - 1 - z
        reach = line - 1 - pos
        t = j - 2 * (pos - 1)

        @pl.when(pos == 0)
        def _():
            @pl.when(j < plain - late)
            def _():
                pass_range(lent + j, 0, line - 1, up, True)

            @pl.when(j == plain - 1)
            def _():
                pass_late(0, late, up)

            @pl.when(j == plain + 1)
            def _():
                pass_late(late, late * (line - 1), up)

        @pl.when(pos > 0)
        def _():
            lead = jnp.int32(0)
            for c in range(lent):
                lead = jnp.where(t == ready[c], c + 1, lead)

            @pl.when(lead > 0)
            def _():
                pass_range(lead - 1, 0, reach, up, pos == 1)

            near, nearer = jnp.int32(0), jnp.int32(0)
            for c in range(lent, chunks - late):
                near = jnp.where(t == ready[c], c + 1, near)
                nearer = jnp.where(t == ready[c] + 1, c + 1, nearer)

            @pl.when((near > 0) & (reach > 0))
            def _():
                pass_on(near - 1, 0, up, False)

            @pl.when(nearer > 0)
            def _():
                pass_range(nearer - 1, 1, reach, up, False)

            k = t - (work - 1)

            @pl.when((k >= 0) & (k < late * reach))
            def _():
                pass_on(chunks - late + k % late, k // late, up, False)

    def finish(i):
        @pl.when(jnp.logical_not(low) & jnp.logical_not(borrows_low & (i < lent)))
        def _():
            z_copy(i, z, True).wait_recv()

        @pl.when(jnp.logical_not(high) & jnp.logical_not(borrows_high & (i < lent)))
        def _():
            z_copy(i, z, False).wait_recv()

        def total(yy):
            return part[i, z, yy].astype(F32) + rzp[i, z, yy].astype(F32) + rzm[i, z, yy].astype(F32)

        part[i, z, other] = total(other).astype(BF16)
        y_copy(i).start()
        put(i, y, total(y))

    def put(i, half, rows):
        kwg_ref[:, cols(half, i, PAIR * NOPE)] = rows[:, :PAIR * NOPE]
        vwg_ref[:, cols(half, i, GW)] = rows[:, PAIR * NOPE:]

    def close(i, carry):
        y_copy(i).wait_recv()
        put(i, other, yr[i].astype(F32))
        return carry

    def latent_twin():
        l1s[...] = lgacc[:, :, 1 - core].astype(BF16)
        l1_copy().start()

    def latent_send():
        l1_copy().wait_recv()
        twos[...] = lgacc[:, :, core] + l1r[...].astype(F32)
        for k in range(1, chips):
            xs[k - 1] = twos[:, (chip + k) % chips].astype(BF16)
        for p in PAIRS:
            @pl.when(gets_from(p - 1))
            def _():
                for k in range(1, chips):
                    x_copy(k, p).start()

    def latent_pass():
        for p in PAIRS:
            @pl.when(gets_from(p - 1))
            def _():
                for k in range(1, chips):
                    x_copy(k, p).wait_recv()
                for b in (2 * p, 2 * p + 1):
                    tot = twos[b, chip]
                    for k in range(1, chips):
                        tot = tot + xr[k - 1, b].astype(F32)
                    if b == 2:
                        lgown[...] = tot
                    else:
                        l2s[b] = tot.astype(BF16)
                        l2_copy(b).start()

    def latent_gather():
        for b in range(SPAN):
            if b != 2:
                @pl.when(sends_to(b // 2 - 1))
                def _():
                    l2_copy(b).wait_recv()
                    lgown[...] += l2r[b].astype(F32)
        hb[h] = lgown[...].astype(BF16)
        for k in range(1, hn):
            h_copy(k, h).start()

    def latent_out():
        for k in range(1, hn):
            h_copy(k, (h + k) % hn).wait_recv()
        lg_ref[...] = jnp.transpose(hb[...].astype(F32).reshape(tok, width))

    enter()
    last = max(done.values()) + 1

    def turn(j, carry):
        c = jnp.where(edge, lent + j, pick([c for c, _ in turns], j))
        is_lent = inner & (pick([f for _, f in turns], j) > 0)
        active = (j < jnp.where(edge, plain, work)) & (borrows | jnp.logical_not(is_lent))

        @pl.when(active)
        def _():
            compute(c, is_lent)

        @pl.when(edge & (j < lent - 1))
        def _():
            lend_mate(j + 1)

        spent = jnp.where(edge, plain - 1, work - 1)

        @pl.when(j == spent)
        def _():
            latent_twin()

        @pl.when(j == spent + 1)
        def _():
            latent_send()

        @pl.when((j == spent + 2) & edge)
        def _():
            latent_pass()

        for up in (True, False):
            relay(j, up)

        @pl.when((j == spent + late * (line - 2) - 1) & inner)
        def _():
            latent_pass()

        fin = jnp.int32(0)
        for i in range(chunks):
            fin = jnp.where(j == done[i], i + 1, fin)

        @pl.when(fin > 0)
        def _():
            finish(fin - 1)

        @pl.when(edge & (fin > 0) & (fin <= lent))
        def _():
            for k in range(2):
                a_lent(fin - 1, k).wait_recv()
            a_swap(fin - 1, y).start()
            att_ref[:, cols(y, fin - 1, GW)] = atts[fin - 1, 0]

        @pl.when(j == last - late - 1)
        def _():
            lax.fori_loop(0, chunks - late, close, 0)

        return carry

    lax.fori_loop(0, last, turn, 0)
    latent_gather()
    lax.fori_loop(chunks - late, chunks, close, 0)
    latent_out()

    for k in range(1, hn):
        h_copy(k, h).wait_send()
    l1_copy().wait_send()
    for k in range(1, chips):
        for p in PAIRS:
            @pl.when(gets_from(p - 1))
            def _():
                x_copy(k, p).wait_send()
    for b in range(SPAN):
        if b != 2:
            @pl.when(gets_from(b // 2 - 1))
            def _():
                l2_copy(b).wait_send()

    def drain(j, carry):
        y_copy(j).wait_send()
        a_swap(j, other).wait_recv()
        a_swap(j, y).wait_send()
        q_swap(j).wait_send()
        g_swap(j).wait_send()
        for d in range(line):
            @pl.when((d > z) & jnp.logical_not(low & (j < lent)))
            def _():
                z_copy(j, d, True).wait_send()

            @pl.when((d < z) & jnp.logical_not(high & (j < lent)))
            def _():
                z_copy(j, d, False).wait_send()
        return carry

    lax.fori_loop(0, chunks, drain, 0)
    for c in range(lent):
        for k in range(2):
            @pl.when(edge)
            def _():
                q_lend(c, k).wait_send()
                g_lend(c, k).wait_send()

            @pl.when(borrows)
            def _():
                a_lent(c, k).wait_send()
    la_copy(0).wait_send()
    lc_copy(3, core).wait_send()
    for k in FAR:
        @pl.when(sends_to(k))
        def _():
            la_copy(k).wait_send()

        @pl.when(gets_from(k))
        def _():
            lb_copy(k).wait_send()
            lc_copy(2 * (k + 1), core).wait_send()
            lc_copy(2 * (k + 1) + 1, core).wait_send()


def flush(*refs):
    sems = refs[-1]
    copies = [pltpu.make_async_copy(refs[k], refs[4 + k], sems.at[k]) for k in range(4)]
    for copy in copies:
        copy.start()
    for copy in copies:
        copy.wait()


def per_device(n, hn, queries, latents, doc_ids, key_weight, value_weight, out_grad):
    tok = latents.shape[0]
    heads = key_weight.shape[1] // NOPE
    chunks = heads // 2 // PAIR
    line = n // 2
    rows = LATENT // n
    lent = plan(chunks, line)[0]
    slots = chunks + lent
    keys = BLOCKS * tok
    width = LATENT + ROPE
    wide = width + 64
    share = tok // hn
    chips = hn // 2
    ids = doc_ids.reshape(1, tok)
    whole = pl.BlockSpec(memory_space=pltpu.VMEM)
    far = pl.BlockSpec(memory_space=pltpu.HBM)
    dma = pltpu.SemaphoreType.DMA
    ring = max(chips - 1, 1)
    att, lg, kwg, vwg = pl.pallas_call(
        functools.partial(kernel, n, hn, chunks),
        out_shape=(
            pltpu.VMEM((tok, heads * VDIM), BF16),
            pltpu.VMEM((width, tok), F32),
            pltpu.VMEM((rows, heads * NOPE), F32),
            pltpu.VMEM((rows, heads * VDIM), F32),
        ),
        in_specs=[far] * 6,
        out_specs=(whole, whole, whole, whole),
        scratch_shapes=[
            pltpu.VMEM((width, tok), BF16),
            pltpu.VMEM((1, tok), jnp.int32),
            pltpu.VMEM((SPAN, 2, tok // 2, wide), BF16),
            pltpu.VMEM((LATENT, SPAN * tok), BF16),
            pltpu.VMEM((2, keys, 2 * tok), F32),
            pltpu.VMEM((SPAN, chips, 2, share, width), F32),
            pltpu.VMEM((chunks, LATENT, WW), BF16),
            pltpu.VMEM((slots, 2, tok, QW), BF16),
            pltpu.VMEM((slots, 2, tok, GW), BF16),
            pltpu.VMEM((slots, 2, tok, GW), BF16),
            pltpu.VMEM((chunks, line, 2, rows, WW), BF16),
            pltpu.VMEM((chunks, line, 2, rows, WW), BF16),
            pltpu.VMEM((chunks, line, 2, rows, WW), BF16),
            pltpu.VMEM((chunks, rows, WW), BF16),
            pltpu.VMEM((SPAN, chips, share, width), BF16),
            pltpu.VMEM((SPAN, chips, share, width), BF16),
            pltpu.VMEM((SPAN, chips, share, width), F32),
            pltpu.VMEM((ring, SPAN, share, width), BF16),
            pltpu.VMEM((ring, SPAN, share, width), BF16),
            pltpu.VMEM((SPAN, share, width), BF16),
            pltpu.VMEM((SPAN, share, width), BF16),
            pltpu.VMEM((share, width), F32),
            pltpu.VMEM((hn, share, width), BF16),
            dma((2,)), dma((chunks, 2)), dma((chunks,)), dma((chunks,)),
            dma((chunks,)), dma((chunks,)), dma((chunks,)), dma((chunks,)),
            dma((lent, 2)), dma((lent, 2)), dma((lent, 2)), dma((lent, 2)),
            dma((slots, 2)), dma((chunks,)), dma((lent, 2)),
            dma((BACK + 2,)), dma((BACK + 2,)), dma((BACK + 2,)), dma((BACK + 2,)), dma((SPAN,)), dma((SPAN,)),
            dma((chunks, line)), dma((chunks, line)), dma((chunks, line)), dma((chunks, line)),
            dma((chunks,)), dma((chunks,)),
            dma((1,)), dma((1,)), dma((ring, SPAN // 2)), dma((ring, SPAN // 2)), dma((SPAN,)), dma((SPAN,)),
            dma((max(hn - 1, 1),)), dma((hn,)),
        ],
        compiler_params=pltpu.CompilerParams(
            collective_id=0,
            has_side_effects=True,
            vmem_limit_bytes=VMEM_LIMIT,
        ),
    )(latents.T, ids, queries, out_grad, key_weight, value_weight)
    out = (att, lg, kwg, vwg)
    att, lg, kwg, vwg = pl.pallas_call(
        flush,
        out_shape=tuple(pltpu.HBM(o.shape, o.dtype) for o in out),
        in_specs=[whole] * 4,
        out_specs=(far,) * 4,
        scratch_shapes=[dma((4,))],
        compiler_params=pltpu.CompilerParams(vmem_limit_bytes=1024 * 1024),
    )(*out)
    return att, lg.T, kwg, vwg


def solution(mesh):
    in_specs = (
        P("seq", "head"),
        P("seq", None),
        P("seq"),
        P(None, "head"),
        P(None, "head"),
        P("seq", "head"),
    )
    out_specs = (P("seq", "head"), P("seq", None), P("seq", "head"), P("seq", "head"))
    body = functools.partial(per_device, mesh.shape["seq"], mesh.shape["head"])
    return jax.shard_map(
        body, mesh=mesh, in_specs=in_specs, out_specs=out_specs, check_vma=False
    )
```

```python
import functools
import math

import jax
import jax.numpy as jnp
from jax import lax
from jax.experimental import pallas as pl
from jax.experimental.pallas import tpu as pltpu
from jax.sharding import PartitionSpec as P

NOPE = 128
ROPE = 64
VDIM = 128
LATENT = 512
REACH = 4
PAIR = 2
LEND = 3
LATE = 2
VMEM_LIMIT = 60 * 1024 * 1024
MESH = pl.DeviceIdType.MESH
F32 = jnp.float32
BF16 = jnp.bfloat16
BACK = REACH // 2
BLOCKS = 2 * (BACK + 1)
SPAN = BLOCKS + 2
QW = PAIR * (NOPE + ROPE)
GW = PAIR * VDIM
WW = PAIR * (NOPE + VDIM)


def dot(a, b, ca, cb):
    return lax.dot_general(a, b, (((ca,), (cb,)), ((), ())), preferred_element_type=F32)


def pick(table, t):
    out = jnp.int32(0)
    for k, v in enumerate(table):
        if v:
            out = out + jnp.where(t == k, v, 0)
    return out


def plan(chunks, line):
    lent = max(1, chunks * LEND // 8)
    plain = chunks - lent
    late = min(LATE, plain)
    order = [("L", c) for c in range(max(1, lent - 1))] + [("N", lent)]
    order += [("L", c) for c in range(max(1, lent - 1), lent)] + [("N", c) for c in range(lent + 1, chunks)]
    turns, ready, own = [], {}, {}
    for kind, c in order:
        own[c] = len(turns)
        turns.append((c, 0))
        if kind == "L":
            turns.append((c, 1))
        ready[c] = len(turns) - 1
    work = len(turns)
    tail = work - 1 + max(late * (line - 2), 2 * (line - 3) + late - 1) + 1
    done = {}
    for c in range(chunks):
        late_rank = c - (chunks - late)
        done[c] = ready[c] + 2 * (line - 2) if late_rank < 0 else tail + late_rank
    assert len(set(done.values())) == chunks
    return lent, plain, late, turns, ready, [c for _, c in order], done


def kernel(
    n, hn, chunks,
    lat_hbm, qid_hbm, q_ref, g_ref, kw_ref, vw_ref,
    att_ref, lg_ref, kwg_ref, vwg_ref,
    lat_ref, qid_ref, lat_all, lat_t, bias, lgacc, wb, qb, gb, atts, part, rzp, rzm, yr,
    l1s, l1r, twos, xs, xr, l2s, l2r, lgown, hb,
    in_ls, w_ls, q_ls, g_ls, q_ss, q_rs, g_ss, g_rs, qe_ss, qe_rs, ge_ss, ge_rs, a_ss, a_rs, ae_rs,
    la_ss, la_rs, lb_ss, lb_rs, lc_ss, lc_rs,
    zp_ss, zm_ss, zp_rs, zm_rs, y_ss, y_rs, l1_ss, l1_rs, x_ss, x_rs, l2_ss, l2_rs, h_ss, h_rs,
):
    s = lax.axis_index("seq")
    h = lax.axis_index("head")
    line = n // 2
    lent, plain, late, turns, ready, order, done = plan(chunks, line)
    work = len(turns)
    z, y = s // 2, s % 2
    other = 1 - y
    mate = s + 1 - 2 * y
    core = h % 2
    twin = h + 1 - 2 * core
    chips = hn // 2
    chip = h // 2
    tok = lat_ref.shape[1]
    width = LATENT + ROPE
    keys = BLOCKS * tok
    queries = 2 * tok
    to_log2 = 1.0 / math.log(2.0)
    scale = 1.0 / math.sqrt(NOPE + ROPE)
    low, high = z == 0, z == line - 1
    edge = low | high
    inner = jnp.logical_not(edge)
    borrows_low, borrows_high = z == 1, z == line - 2
    borrows = borrows_low | borrows_high
    step = jnp.where(low | borrows_high, 2, -2)

    def remote(src, dst, ss, rs, to):
        return pltpu.make_async_remote_copy(
            src_ref=src, dst_ref=dst, send_sem=ss, recv_sem=rs, device_id=to, device_id_type=MESH
        )

    def cols(half, j, wide):
        return pl.ds(pl.multiple_of(half * (chunks * wide) + j * wide, 128), wide)

    def w_copy(j, which):
        ref, col, wide = (kw_ref, 0, PAIR * NOPE) if which == 0 else (vw_ref, PAIR * NOPE, GW)
        return pltpu.make_async_copy(
            ref.at[:, cols(y, j, wide)], wb.at[j, :, pl.ds(col, wide)], w_ls.at[j, which]
        )

    def q_own(j):
        return pltpu.make_async_copy(q_ref.at[:, cols(y, j, QW)], qb.at[j, 0], q_ls.at[j])

    def g_own(j):
        return pltpu.make_async_copy(g_ref.at[:, cols(y, j, GW)], gb.at[j, 0], g_ls.at[j])

    def q_swap(j):
        return remote(q_ref.at[:, cols(other, j, QW)], qb.at[j, 1], q_ss.at[j], q_rs.at[j], (mate, h))

    def g_swap(j):
        return remote(g_ref.at[:, cols(other, j, GW)], gb.at[j, 1], g_ss.at[j], g_rs.at[j], (mate, h))

    def q_lend(c, k):
        src = q_ref.at[:, cols(y, c, QW)] if k == 0 else qb.at[c, 1]
        return remote(src, qb.at[chunks + c, k], qe_ss.at[c, k], qe_rs.at[c, k], (s + step, h))

    def g_lend(c, k):
        src = g_ref.at[:, cols(y, c, GW)] if k == 0 else gb.at[c, 1]
        return remote(src, gb.at[chunks + c, k], ge_ss.at[c, k], ge_rs.at[c, k], (s + step, h))

    def a_swap(j, half):
        return remote(atts.at[j, 1], att_ref.at[:, cols(half, j, GW)], a_ss.at[j, 1], a_rs.at[j], (mate, h))

    def a_lent(c, k):
        return remote(atts.at[chunks + c, k], atts.at[c, k], a_ss.at[chunks + c, k], ae_rs.at[c, k], (s + step, h))

    def la_copy(k):
        to, b = (mate, 3) if k == 0 else (s + 2 * k, 2 * (k + 1))
        return remote(lat_all.at[2, core], lat_all.at[b, core], la_ss.at[k + 1], la_rs.at[k + 1], (to, h))

    def lb_copy(k):
        b = 2 * (k + 1)
        return remote(lat_all.at[b, core], lat_all.at[b + 1, core], lb_ss.at[k + 1], lb_rs.at[k + 1], (mate, h))

    def lc_copy(b, half):
        return remote(lat_all.at[b, half], lat_all.at[b, half], lc_ss.at[b], lc_rs.at[b], (s, twin))

    def sends_to(k):
        return high if k < 0 else z + k < line

    def gets_from(k):
        return borrows_high if k < 0 else z - k >= 0

    PAIRS = [p for p in range(SPAN // 2 - 1, -1, -1) if p != 1] + [1]
    FAR = [k for k in range(-1, BACK + 1) if k != 0]

    def z_copy(i, d, up):
        buf, ss, rs = (rzp, zp_ss, zp_rs) if up else (rzm, zm_ss, zm_rs)
        return remote(part.at[i, d], buf.at[i, d], ss.at[i, d], rs.at[i, d], (s + 2 if up else s - 2, h))

    def y_copy(i):
        return remote(part.at[i, z, other], yr.at[i], y_ss.at[i], y_rs.at[i], (mate, h))

    def l1_copy():
        return remote(l1s, l1r, l1_ss.at[0], l1_rs.at[0], (s, twin))

    def x_copy(k, p):
        at = pl.ds(2 * p, 2)
        return remote(
            xs.at[k - 1, at], xr.at[k - 1, at], x_ss.at[k - 1, p], x_rs.at[k - 1, p], (s, (h + 2 * k) % hn)
        )

    def l2_copy(b):
        base = s if b % 2 == 0 else mate
        hops = b // 2 - 1
        if b >= SPAN - 2:
            base, hops = jnp.where(high, s, base), jnp.where(high, 1, hops)
        return remote(l2s.at[b], l2r.at[b], l2_ss.at[b], l2_rs.at[b], (base - 2 * hops, h))

    def h_copy(k, slot):
        return remote(hb.at[slot], hb.at[slot], h_ss.at[k - 1], h_rs.at[slot], (s, (h + k) % hn))

    def lend_mate(c):
        q_swap(c).wait_recv()
        g_swap(c).wait_recv()
        q_lend(c, 1).start()
        g_lend(c, 1).start()

    def enter():
        loads = [
            pltpu.make_async_copy(src, dst, in_ls.at[k])
            for k, (src, dst) in enumerate(((lat_hbm, lat_ref), (qid_hbm, qid_ref)))
        ]
        for load in loads:
            load.start()
        barrier = pltpu.get_barrier_semaphore()

        def greet(to):
            pl.semaphore_signal(barrier, inc=1, device_id=to, device_id_type=MESH)

        greet((mate, h))
        for k in range(1, BACK + 1):
            @pl.when(z + k < line)
            def _():
                greet((s + 2 * k, h))
                greet((mate + 2 * k, h))

            @pl.when(z - k >= 0)
            def _():
                greet((s - 2 * k, h))
                greet((mate - 2 * k, h))
        for k in range(1, hn):
            greet((s, (h + k) % hn))
        for load in loads:
            load.wait()
        ids = jnp.transpose(jnp.broadcast_to(qid_ref[...].astype(F32), (tok, tok)))
        mine = jnp.transpose(lat_ref[...].astype(F32))
        packed = jnp.concatenate([mine, ids[:, :lat_all.shape[3] - width]], axis=1).astype(BF16)
        lat_all[2] = packed.reshape(lat_all.shape[1:])
        pl.semaphore_wait(barrier, 2 * (jnp.minimum(z, BACK) + jnp.minimum(line - 1 - z, BACK)) + hn)
        la_copy(0).start()
        for k in FAR:
            @pl.when(sends_to(k))
            def _():
                la_copy(k).start()

        def fetch(c):
            w_copy(c, 0).start()
            w_copy(c, 1).start()
            q_own(c).start()
            g_own(c).start()

        def swap(c):
            q_swap(c).start()
            g_swap(c).start()

        @pl.when(edge)
        def _():
            q_swap(0).start()
            for c in range(min(2, lent)):
                q_lend(c, 0).start()
                g_lend(c, 0).start()
            for c in range(lent, chunks):
                fetch(c)

        @pl.when(inner)
        def _():
            for c in order:
                fetch(c)
            q_swap(order[0]).start()

        lgacc[...] = jnp.zeros_like(lgacc)
        zero = jnp.zeros(part.shape[1:], BF16)

        def clear(i, c):
            part[i] = zero
            return c

        lax.fori_loop(0, chunks, clear, 0)
        for cond, buf, d, count in (
            (low, rzp, 0, chunks), (borrows_low, rzp, 1, lent),
            (high, rzm, line - 1, chunks), (borrows_high, rzm, line - 2, lent),
        ):
            @pl.when(cond)
            def _():
                for i in range(count):
                    buf[i, d] = jnp.zeros(buf.shape[2:], BF16)

        for k in FAR:
            @pl.when(gets_from(k))
            def _():
                la_copy(k).wait_recv()
                lb_copy(k).start()
                lc_copy(2 * (k + 1), core).start()

            @pl.when(jnp.logical_not(gets_from(k)))
            def _():
                for b in (2 * (k + 1), 2 * (k + 1) + 1):
                    lat_all[b] = jnp.zeros(lat_all.shape[1:], BF16)
        g_swap(0).start()
        la_copy(0).wait_recv()
        lc_copy(3, core).start()
        for k in FAR:
            @pl.when(gets_from(k))
            def _():
                lb_copy(k).wait_recv()
                lc_copy(2 * (k + 1) + 1, core).start()

        @pl.when(edge)
        def _():
            for c in range(max(lent, plain)):
                if c < plain:
                    swap(lent + c)
                if c + 1 < lent:
                    swap(c + 1)
            lend_mate(0)
            for c in range(2, lent):
                q_lend(c, 0).start()
                g_lend(c, 0).start()

        @pl.when(inner)
        def _():
            for c in order[1:]:
                swap(c)

        lc_copy(3, 1 - core).wait_recv()
        for k in FAR:
            @pl.when(gets_from(k))
            def _():
                lc_copy(2 * (k + 1), 1 - core).wait_recv()
                lc_copy(2 * (k + 1) + 1, 1 - core).wait_recv()
        for b in range(SPAN):
            rows = lat_all[b].reshape(tok, lat_all.shape[3])
            lat_t[:, b * tok:(b + 1) * tok] = jnp.transpose(rows[:, :LATENT])

        def ids_of(b):
            tail = lat_all[b].reshape(tok, lat_all.shape[3])[:, LATENT:].astype(F32)
            return jnp.transpose(tail)[ROPE:ROPE + 1, :]

        row = lax.broadcasted_iota(jnp.int32, (tok, tok), 0)
        col = lax.broadcasted_iota(jnp.int32, (tok, tok), 1)

        def mask(which, window, query_at, shift):
            for k in range(2):
                query_id = ids_of(query_at + k)
                for b in range(BLOCKS):
                    back = window // 2 - 1 + b // 2
                    block = (s if b % 2 == 0 else mate) - 2 * back
                    rows = lat_all[window + b].reshape(tok, lat_all.shape[3])
                    key_id = rows[:, width:width + 1].astype(F32)
                    first = (s if k == 0 else mate) + shift - block
                    visible = (row <= col + first * tok) & (block >= 0) & (key_id == query_id)
                    bias[which, b * tok:(b + 1) * tok, k * tok:(k + 1) * tok] = jnp.where(visible, 0.0, -jnp.inf)

        mask(0, 2, 2, 0)

        @pl.when(borrows_low)
        def _():
            mask(1, 2, 4, -2)

        @pl.when(borrows_high)
        def _():
            mask(1, 0, 0, 2)

    def compute(c, is_lent):
        slot = jnp.where(is_lent, chunks + c, c)
        which = jnp.where(is_lent, 1, 0)
        window = jnp.where(is_lent & borrows_high, 0, 2)

        @pl.when(jnp.logical_not(is_lent))
        def _():
            w_copy(c, 0).wait()
            w_copy(c, 1).wait()
            q_own(c).wait()
            g_own(c).wait()
            q_swap(c).wait_recv()
            g_swap(c).wait_recv()

        @pl.when(is_lent)
        def _():
            for k in range(2):
                q_lend(c, k).wait_recv()
                g_lend(c, k).wait_recv()

        rows = lat_all[pl.ds(window, BLOCKS)].reshape(keys, lat_all.shape[3])
        lat = rows[:, :LATENT]
        rope = rows[:, LATENT:width]
        w = wb[c]
        q2 = qb[slot].reshape(queries, QW)
        g2 = gb[slot].reshape(queries, GW)
        kv = dot(lat, w, 1, 0).astype(BF16)
        dks, dvs, rope_sum = [], [], None
        for a in range(PAIR):
            q = q2[:, a * (NOPE + ROPE):(a + 1) * (NOPE + ROPE)]
            g = g2[:, a * VDIM:(a + 1) * VDIM]
            v = kv[:, PAIR * NOPE + a * VDIM:PAIR * NOPE + (a + 1) * VDIM]
            k = jnp.concatenate([kv[:, a * NOPE:(a + 1) * NOPE], rope], axis=1)
            sc = dot(k, q, 1, 1) * (scale * to_log2) + bias[which]
            e = jnp.exp2(sc - jnp.max(sc, axis=0, keepdims=True))
            p = e * (1.0 / jnp.sum(e, axis=0, keepdims=True))
            pb = p.astype(BF16)
            att = jnp.transpose(dot(v, pb, 0, 0)).astype(BF16)
            for k in range(2):
                atts[slot, k, :, a * VDIM:(a + 1) * VDIM] = att[k * tok:(k + 1) * tok]
            dp = dot(v, g, 1, 1)
            delta = jnp.sum(p * dp, axis=0, keepdims=True)
            ds = (p * (dp - delta) * scale).astype(BF16)
            dk = dot(ds, q, 1, 0)
            dvs.append(dot(pb, g, 1, 0).astype(BF16))
            dks.append(dk[:, :NOPE].astype(BF16))
            r = dk[:, NOPE:]
            rope_sum = r if rope_sum is None else rope_sum + r
        dd = jnp.concatenate(dks + dvs, axis=1)
        lat_cols = lat_t[:, pl.ds(pl.multiple_of(window * tok, 128), keys)]
        grad = dot(lat_cols, dd, 1, 0).reshape(part.shape[1:])
        part[c] = (part[c].astype(F32) + grad).astype(BF16)
        flat = (BLOCKS,) + lgacc.shape[1:4]
        at = pl.ds(window, BLOCKS)
        lgacc[at, :, :, :, :LATENT] += dot(dd, w, 1, 1).reshape(*flat, LATENT)
        lgacc[at, :, :, :, LATENT:] += rope_sum.reshape(*flat, ROPE)

        @pl.when(is_lent)
        def _():
            for k in range(2):
                a_lent(c, k).start()

        @pl.when(jnp.logical_not(is_lent))
        def _():
            a_swap(c, y).start()
            att_ref[:, cols(y, c, GW)] = atts[c, 0]

    def pass_on(i, r, up, first):
        d = line - 1 - r if up else r

        @pl.when(jnp.logical_not(first))
        def _():
            z_copy(i, d, up).wait_recv()
            buf = rzp if up else rzm
            part[i, d] = (part[i, d].astype(F32) + buf[i, d].astype(F32)).astype(BF16)

        z_copy(i, d, up).start()

    def pass_range(i, r0, r1, up, first):
        def one(r, c):
            pass_on(i, r, up, first)
            return c

        lax.fori_loop(r0, r1, one, 0)

    def pass_late(k0, k1, up):
        def one(k, c):
            pass_on(chunks - late + k % late, k // late, up, True)
            return c

        lax.fori_loop(k0, k1, one, 0)

    def relay(j, up):
        pos = z if up else line - 1 - z
        reach = line - 1 - pos
        t = j - 2 * (pos - 1)

        @pl.when(pos == 0)
        def _():
            @pl.when(j < plain - late)
            def _():
                pass_range(lent + j, 0, line - 1, up, True)

            @pl.when(j == plain - 1)
            def _():
                pass_late(0, late * (line - 1), up)

        @pl.when(pos > 0)
        def _():
            lead = jnp.int32(0)
            for c in range(lent):
                lead = jnp.where(t == ready[c], c + 1, lead)

            @pl.when(lead > 0)
            def _():
                pass_range(lead - 1, 0, reach, up, pos == 1)

            near, nearer = jnp.int32(0), jnp.int32(0)
            for c in range(lent, chunks - late):
                near = jnp.where(t == ready[c], c + 1, near)
                nearer = jnp.where(t == ready[c] + 1, c + 1, nearer)

            @pl.when((near > 0) & (reach > 0))
            def _():
                pass_on(near - 1, 0, up, False)

            @pl.when(nearer > 0)
            def _():
                pass_range(nearer - 1, 1, reach, up, False)

            k = t - (work - 1)

            @pl.when((k >= 0) & (k < late * reach))
            def _():
                pass_on(chunks - late + k % late, k // late, up, False)

    def finish(i):
        @pl.when(jnp.logical_not(low) & jnp.logical_not(borrows_low & (i < lent)))
        def _():
            z_copy(i, z, True).wait_recv()

        @pl.when(jnp.logical_not(high) & jnp.logical_not(borrows_high & (i < lent)))
        def _():
            z_copy(i, z, False).wait_recv()

        def total(yy):
            return part[i, z, yy].astype(F32) + rzp[i, z, yy].astype(F32) + rzm[i, z, yy].astype(F32)

        part[i, z, other] = total(other).astype(BF16)
        y_copy(i).start()
        put(i, y, total(y))

    def put(i, half, rows):
        kwg_ref[:, cols(half, i, PAIR * NOPE)] = rows[:, :PAIR * NOPE]
        vwg_ref[:, cols(half, i, GW)] = rows[:, PAIR * NOPE:]

    def close(i, carry):
        y_copy(i).wait_recv()
        put(i, other, yr[i].astype(F32))
        return carry

    def latent_twin():
        l1s[...] = lgacc[:, :, 1 - core].astype(BF16)
        l1_copy().start()

    def latent_send():
        l1_copy().wait_recv()
        twos[...] = lgacc[:, :, core] + l1r[...].astype(F32)
        for k in range(1, chips):
            xs[k - 1] = twos[:, (chip + k) % chips].astype(BF16)
        for p in PAIRS:
            @pl.when(gets_from(p - 1))
            def _():
                for k in range(1, chips):
                    x_copy(k, p).start()

    def latent_pass():
        for p in PAIRS:
            @pl.when(gets_from(p - 1))
            def _():
                for k in range(1, chips):
                    x_copy(k, p).wait_recv()
                for b in (2 * p, 2 * p + 1):
                    tot = twos[b, chip]
                    for k in range(1, chips):
                        tot = tot + xr[k - 1, b].astype(F32)
                    if b == 2:
                        lgown[...] = tot
                    elif 2 * p == SPAN - 4:
                        @pl.when(borrows_high)
                        def _():
                            l2_copy(b + 2).wait_recv()
                            l2s[b] = (tot + l2r[b + 2].astype(F32)).astype(BF16)

                        @pl.when(jnp.logical_not(borrows_high))
                        def _():
                            l2s[b] = tot.astype(BF16)
                        l2_copy(b).start()
                    else:
                        l2s[b] = tot.astype(BF16)
                        l2_copy(b).start()

    def latent_gather():
        for b in range(SPAN):
            if b != 2:
                last_hop = z != line - 3 if b >= SPAN - 2 else z >= 0

                @pl.when(sends_to(b // 2 - 1) & last_hop)
                def _():
                    l2_copy(b).wait_recv()
                    lgown[...] += l2r[b].astype(F32)
        hb[h] = lgown[...].astype(BF16)
        for k in range(1, hn):
            h_copy(k, h).start()

    def latent_out():
        for k in range(1, hn):
            h_copy(k, (h + k) % hn).wait_recv()
        lg_ref[...] = jnp.transpose(hb[...].astype(F32).reshape(tok, width))

    enter()
    last = max(done.values()) + 1

    def turn(j, carry):
        c = jnp.where(edge, lent + j, pick([c for c, _ in turns], j))
        is_lent = inner & (pick([f for _, f in turns], j) > 0)
        active = (j < jnp.where(edge, plain, work)) & (borrows | jnp.logical_not(is_lent))

        @pl.when(active)
        def _():
            compute(c, is_lent)

        @pl.when(edge & (j < lent - 1))
        def _():
            lend_mate(j + 1)

        spent = jnp.where(edge, plain - 1, work - 1)

        @pl.when(j == spent)
        def _():
            latent_twin()

        @pl.when((j == spent + 1) & edge)
        def _():
            latent_send()

        @pl.when((j == spent + 2) & edge)
        def _():
            latent_pass()

        for up in (True, False):
            relay(j, up)

        @pl.when((j == spent + 1) & inner)
        def _():
            latent_send()

        @pl.when((j == spent + late * (line - 2)) & inner)
        def _():
            latent_pass()

        fin = jnp.int32(0)
        for i in range(chunks):
            fin = jnp.where(j == done[i], i + 1, fin)

        @pl.when(fin > 0)
        def _():
            finish(fin - 1)

        @pl.when(edge & (fin > 0) & (fin <= lent))
        def _():
            for k in range(2):
                a_lent(fin - 1, k).wait_recv()
            a_swap(fin - 1, y).start()
            att_ref[:, cols(y, fin - 1, GW)] = atts[fin - 1, 0]

        @pl.when(j == last - late - 1)
        def _():
            lax.fori_loop(0, chunks - late, close, 0)

        return carry

    lax.fori_loop(0, last, turn, 0)
    latent_gather()
    lax.fori_loop(chunks - late, chunks, close, 0)
    latent_out()

    for k in range(1, hn):
        h_copy(k, h).wait_send()
    l1_copy().wait_send()
    for k in range(1, chips):
        for p in PAIRS:
            @pl.when(gets_from(p - 1))
            def _():
                x_copy(k, p).wait_send()
    for b in range(SPAN):
        if b != 2:
            @pl.when(gets_from(b // 2 - 1))
            def _():
                l2_copy(b).wait_send()

    def drain(j, carry):
        y_copy(j).wait_send()
        a_swap(j, other).wait_recv()
        a_swap(j, y).wait_send()
        q_swap(j).wait_send()
        g_swap(j).wait_send()
        for d in range(line):
            @pl.when((d > z) & jnp.logical_not(low & (j < lent)))
            def _():
                z_copy(j, d, True).wait_send()

            @pl.when((d < z) & jnp.logical_not(high & (j < lent)))
            def _():
                z_copy(j, d, False).wait_send()
        return carry

    lax.fori_loop(0, chunks, drain, 0)
    for c in range(lent):
        for k in range(2):
            @pl.when(edge)
            def _():
                q_lend(c, k).wait_send()
                g_lend(c, k).wait_send()

            @pl.when(borrows)
            def _():
                a_lent(c, k).wait_send()
    la_copy(0).wait_send()
    lc_copy(3, core).wait_send()
    for k in FAR:
        @pl.when(sends_to(k))
        def _():
            la_copy(k).wait_send()

        @pl.when(gets_from(k))
        def _():
            lb_copy(k).wait_send()
            lc_copy(2 * (k + 1), core).wait_send()
            lc_copy(2 * (k + 1) + 1, core).wait_send()


def flush(*refs):
    sems = refs[-1]
    copies = [pltpu.make_async_copy(refs[k], refs[4 + k], sems.at[k]) for k in range(4)]
    for copy in copies:
        copy.start()
    for copy in copies:
        copy.wait()


def per_device(n, hn, queries, latents, doc_ids, key_weight, value_weight, out_grad):
    tok = latents.shape[0]
    heads = key_weight.shape[1] // NOPE
    chunks = heads // 2 // PAIR
    line = n // 2
    rows = LATENT // n
    lent = plan(chunks, line)[0]
    slots = chunks + lent
    keys = BLOCKS * tok
    width = LATENT + ROPE
    wide = width + 64
    share = tok // hn
    chips = hn // 2
    ids = doc_ids.reshape(1, tok)
    whole = pl.BlockSpec(memory_space=pltpu.VMEM)
    far = pl.BlockSpec(memory_space=pltpu.HBM)
    dma = pltpu.SemaphoreType.DMA
    ring = max(chips - 1, 1)
    att, lg, kwg, vwg = pl.pallas_call(
        functools.partial(kernel, n, hn, chunks),
        out_shape=(
            pltpu.VMEM((tok, heads * VDIM), BF16),
            pltpu.VMEM((width, tok), F32),
            pltpu.VMEM((rows, heads * NOPE), F32),
            pltpu.VMEM((rows, heads * VDIM), F32),
        ),
        in_specs=[far] * 6,
        out_specs=(whole, whole, whole, whole),
        scratch_shapes=[
            pltpu.VMEM((width, tok), BF16),
            pltpu.VMEM((1, tok), jnp.int32),
            pltpu.VMEM((SPAN, 2, tok // 2, wide), BF16),
            pltpu.VMEM((LATENT, SPAN * tok), BF16),
            pltpu.VMEM((2, keys, 2 * tok), F32),
            pltpu.VMEM((SPAN, chips, 2, share, width), F32),
            pltpu.VMEM((chunks, LATENT, WW), BF16),
            pltpu.VMEM((slots, 2, tok, QW), BF16),
            pltpu.VMEM((slots, 2, tok, GW), BF16),
            pltpu.VMEM((slots, 2, tok, GW), BF16),
            pltpu.VMEM((chunks, line, 2, rows, WW), BF16),
            pltpu.VMEM((chunks, line, 2, rows, WW), BF16),
            pltpu.VMEM((chunks, line, 2, rows, WW), BF16),
            pltpu.VMEM((chunks, rows, WW), BF16),
            pltpu.VMEM((SPAN, chips, share, width), BF16),
            pltpu.VMEM((SPAN, chips, share, width), BF16),
            pltpu.VMEM((SPAN, chips, share, width), F32),
            pltpu.VMEM((ring, SPAN, share, width), BF16),
            pltpu.VMEM((ring, SPAN, share, width), BF16),
            pltpu.VMEM((SPAN, share, width), BF16),
            pltpu.VMEM((SPAN, share, width), BF16),
            pltpu.VMEM((share, width), F32),
            pltpu.VMEM((hn, share, width), BF16),
            dma((2,)), dma((chunks, 2)), dma((chunks,)), dma((chunks,)),
            dma((chunks,)), dma((chunks,)), dma((chunks,)), dma((chunks,)),
            dma((lent, 2)), dma((lent, 2)), dma((lent, 2)), dma((lent, 2)),
            dma((slots, 2)), dma((chunks,)), dma((lent, 2)),
            dma((BACK + 2,)), dma((BACK + 2,)), dma((BACK + 2,)), dma((BACK + 2,)), dma((SPAN,)), dma((SPAN,)),
            dma((chunks, line)), dma((chunks, line)), dma((chunks, line)), dma((chunks, line)),
            dma((chunks,)), dma((chunks,)),
            dma((1,)), dma((1,)), dma((ring, SPAN // 2)), dma((ring, SPAN // 2)), dma((SPAN,)), dma((SPAN,)),
            dma((max(hn - 1, 1),)), dma((hn,)),
        ],
        compiler_params=pltpu.CompilerParams(
            collective_id=0,
            has_side_effects=True,
            vmem_limit_bytes=VMEM_LIMIT,
        ),
    )(latents.T, ids, queries, out_grad, key_weight, value_weight)
    out = (att, lg, kwg, vwg)
    att, lg, kwg, vwg = pl.pallas_call(
        flush,
        out_shape=tuple(pltpu.HBM(o.shape, o.dtype) for o in out),
        in_specs=[whole] * 4,
        out_specs=(far,) * 4,
        scratch_shapes=[dma((4,))],
        compiler_params=pltpu.CompilerParams(vmem_limit_bytes=1024 * 1024),
    )(*out)
    return att, lg.T, kwg, vwg


def solution(mesh):
    in_specs = (
        P("seq", "head"),
        P("seq", None),
        P("seq"),
        P(None, "head"),
        P(None, "head"),
        P("seq", "head"),
    )
    out_specs = (P("seq", "head"), P("seq", None), P("seq", "head"), P("seq", "head"))
    body = functools.partial(per_device, mesh.shape["seq"], mesh.shape["head"])
    return jax.shard_map(
        body, mesh=mesh, in_specs=in_specs, out_specs=out_specs, check_vma=False
    )
```

```python
import functools
import math

import jax
import jax.numpy as jnp
from jax import lax
from jax.experimental import pallas as pl
from jax.experimental.pallas import tpu as pltpu
from jax.sharding import PartitionSpec as P

NOPE = 128
ROPE = 64
VDIM = 128
LATENT = 512
REACH = 4
PAIR = 2
LEND = 3
LATE = 2
VMEM_LIMIT = 60 * 1024 * 1024
MESH = pl.DeviceIdType.MESH
F32 = jnp.float32
BF16 = jnp.bfloat16
BACK = REACH // 2
BLOCKS = 2 * (BACK + 1)
SPAN = BLOCKS + 2
QW = PAIR * (NOPE + ROPE)
GW = PAIR * VDIM
WW = PAIR * (NOPE + VDIM)


def dot(a, b, ca, cb):
    return lax.dot_general(a, b, (((ca,), (cb,)), ((), ())), preferred_element_type=F32)


def pick(table, t):
    out = jnp.int32(0)
    for k, v in enumerate(table):
        if v:
            out = out + jnp.where(t == k, v, 0)
    return out


def plan(chunks, line):
    lent = max(1, chunks * LEND // 8)
    plain = chunks - lent
    late = min(LATE, plain)
    order = [("L", c) for c in range(max(1, lent - 1))] + [("N", lent)]
    order += [("L", c) for c in range(max(1, lent - 1), lent)] + [("N", c) for c in range(lent + 1, chunks)]
    turns, ready, own = [], {}, {}
    for kind, c in order:
        own[c] = len(turns)
        turns.append((c, 0))
        if kind == "L":
            turns.append((c, 1))
        ready[c] = len(turns) - 1
    work = len(turns)
    tail = work - 1 + max(late * (line - 2), 2 * (line - 3) + late - 1) + 1
    done = {}
    for c in range(chunks):
        late_rank = c - (chunks - late)
        done[c] = ready[c] + 2 * (line - 2) + 1 if late_rank < 0 else tail + late_rank
    assert len(set(done.values())) == chunks
    return lent, plain, late, turns, ready, [c for _, c in order], done


def kernel(
    n, hn, chunks,
    lat_hbm, qid_hbm, q_ref, g_ref, kw_ref, vw_ref,
    att_ref, lg_ref, kwg_ref, vwg_ref,
    lat_ref, qid_ref, lat_all, lat_t, bias, lgacc, wb, qb, gb, atts, part, rzp, rzm, yr,
    l1s, l1r, twos, xs, xr, l2s, l2r, lgown, hb,
    in_ls, w_ls, q_ls, g_ls, q_ss, q_rs, g_ss, g_rs, qe_ss, qe_rs, ge_ss, ge_rs, a_ss, a_rs, ae_rs,
    la_ss, la_rs, lb_ss, lb_rs, lc_ss, lc_rs,
    zp_ss, zm_ss, zp_rs, zm_rs, y_ss, y_rs, l1_ss, l1_rs, x_ss, x_rs, l2_ss, l2_rs, h_ss, h_rs,
):
    s = lax.axis_index("seq")
    h = lax.axis_index("head")
    line = n // 2
    lent, plain, late, turns, ready, order, done = plan(chunks, line)
    work = len(turns)
    z, y = s // 2, s % 2
    other = 1 - y
    mate = s + 1 - 2 * y
    core = h % 2
    twin = h + 1 - 2 * core
    chips = hn // 2
    chip = h // 2
    tok = lat_ref.shape[1]
    width = LATENT + ROPE
    keys = BLOCKS * tok
    queries = 2 * tok
    to_log2 = 1.0 / math.log(2.0)
    scale = 1.0 / math.sqrt(NOPE + ROPE)
    low, high = z == 0, z == line - 1
    edge = low | high
    inner = jnp.logical_not(edge)
    borrows_low, borrows_high = z == 1, z == line - 2
    borrows = borrows_low | borrows_high
    step = jnp.where(low | borrows_high, 2, -2)

    def remote(src, dst, ss, rs, to):
        return pltpu.make_async_remote_copy(
            src_ref=src, dst_ref=dst, send_sem=ss, recv_sem=rs, device_id=to, device_id_type=MESH
        )

    def cols(half, j, wide):
        return pl.ds(pl.multiple_of(half * (chunks * wide) + j * wide, 128), wide)

    def w_copy(j, which):
        ref, col, wide = (kw_ref, 0, PAIR * NOPE) if which == 0 else (vw_ref, PAIR * NOPE, GW)
        return pltpu.make_async_copy(
            ref.at[:, cols(y, j, wide)], wb.at[j, :, pl.ds(col, wide)], w_ls.at[j, which]
        )

    def q_own(j):
        return pltpu.make_async_copy(q_ref.at[:, cols(y, j, QW)], qb.at[j, 0], q_ls.at[j])

    def g_own(j):
        return pltpu.make_async_copy(g_ref.at[:, cols(y, j, GW)], gb.at[j, 0], g_ls.at[j])

    def q_swap(j):
        return remote(q_ref.at[:, cols(other, j, QW)], qb.at[j, 1], q_ss.at[j], q_rs.at[j], (mate, h))

    def g_swap(j):
        return remote(g_ref.at[:, cols(other, j, GW)], gb.at[j, 1], g_ss.at[j], g_rs.at[j], (mate, h))

    def q_lend(c, k):
        src = q_ref.at[:, cols(y, c, QW)] if k == 0 else qb.at[c, 1]
        return remote(src, qb.at[chunks + c, k], qe_ss.at[c, k], qe_rs.at[c, k], (s + step, h))

    def g_lend(c, k):
        src = g_ref.at[:, cols(y, c, GW)] if k == 0 else gb.at[c, 1]
        return remote(src, gb.at[chunks + c, k], ge_ss.at[c, k], ge_rs.at[c, k], (s + step, h))

    def a_swap(j, half):
        return remote(atts.at[j, 1], att_ref.at[:, cols(half, j, GW)], a_ss.at[j, 1], a_rs.at[j], (mate, h))

    def a_lent(c, k):
        return remote(atts.at[chunks + c, k], atts.at[c, k], a_ss.at[chunks + c, k], ae_rs.at[c, k], (s + step, h))

    def la_copy(k):
        to, b = (mate, 3) if k == 0 else (s + 2 * k, 2 * (k + 1))
        return remote(lat_all.at[2, core], lat_all.at[b, core], la_ss.at[k + 1], la_rs.at[k + 1], (to, h))

    def lb_copy(k):
        b = 2 * (k + 1)
        return remote(lat_all.at[b, core], lat_all.at[b + 1, core], lb_ss.at[k + 1], lb_rs.at[k + 1], (mate, h))

    def lc_copy(b, half):
        return remote(lat_all.at[b, half], lat_all.at[b, half], lc_ss.at[b], lc_rs.at[b], (s, twin))

    def sends_to(k):
        return high if k < 0 else z + k < line

    def gets_from(k):
        return borrows_high if k < 0 else z - k >= 0

    PAIRS = [p for p in range(SPAN // 2 - 1, -1, -1) if p != 1] + [1]
    FAR = [k for k in range(-1, BACK + 1) if k != 0]

    def z_copy(i, d, up):
        buf, ss, rs = (rzp, zp_ss, zp_rs) if up else (rzm, zm_ss, zm_rs)
        return remote(part.at[i, d], buf.at[i, d], ss.at[i, d], rs.at[i, d], (s + 2 if up else s - 2, h))

    def y_copy(i):
        return remote(part.at[i, z, other], yr.at[i], y_ss.at[i], y_rs.at[i], (mate, h))

    def l1_copy():
        return remote(l1s, l1r, l1_ss.at[0], l1_rs.at[0], (s, twin))

    def x_copy(k, p):
        at = pl.ds(2 * p, 2)
        return remote(
            xs.at[k - 1, at], xr.at[k - 1, at], x_ss.at[k - 1, p], x_rs.at[k - 1, p], (s, (h + 2 * k) % hn)
        )

    def l2_copy(b):
        base = s if b % 2 == 0 else mate
        hops = b // 2 - 1
        if b >= SPAN - 2:
            base, hops = jnp.where(high, s, base), jnp.where(high, 1, hops)
        return remote(l2s.at[b], l2r.at[b], l2_ss.at[b], l2_rs.at[b], (base - 2 * hops, h))

    def h_copy(k, slot):
        return remote(hb.at[slot], hb.at[slot], h_ss.at[k - 1], h_rs.at[slot], (s, (h + k) % hn))

    def lend_mate(c):
        q_swap(c).wait_recv()
        g_swap(c).wait_recv()
        q_lend(c, 1).start()
        g_lend(c, 1).start()

    def enter():
        loads = [
            pltpu.make_async_copy(src, dst, in_ls.at[k])
            for k, (src, dst) in enumerate(((lat_hbm, lat_ref), (qid_hbm, qid_ref)))
        ]
        for load in loads:
            load.start()
        barrier = pltpu.get_barrier_semaphore()

        def greet(to):
            pl.semaphore_signal(barrier, inc=1, device_id=to, device_id_type=MESH)

        greet((mate, h))
        for k in range(1, BACK + 1):
            @pl.when(z + k < line)
            def _():
                greet((s + 2 * k, h))
                greet((mate + 2 * k, h))

            @pl.when(z - k >= 0)
            def _():
                greet((s - 2 * k, h))
                greet((mate - 2 * k, h))
        for k in range(1, hn):
            greet((s, (h + k) % hn))
        for load in loads:
            load.wait()
        ids = jnp.transpose(jnp.broadcast_to(qid_ref[...].astype(F32), (tok, tok)))
        mine = jnp.transpose(lat_ref[...].astype(F32))
        packed = jnp.concatenate([mine, ids[:, :lat_all.shape[3] - width]], axis=1).astype(BF16)
        lat_all[2] = packed.reshape(lat_all.shape[1:])
        pl.semaphore_wait(barrier, 2 * (jnp.minimum(z, BACK) + jnp.minimum(line - 1 - z, BACK)) + hn)
        la_copy(0).start()
        for k in FAR:
            @pl.when(sends_to(k))
            def _():
                la_copy(k).start()

        def fetch(c):
            w_copy(c, 0).start()
            w_copy(c, 1).start()
            q_own(c).start()
            g_own(c).start()

        def swap(c):
            q_swap(c).start()
            g_swap(c).start()

        @pl.when(edge)
        def _():
            q_swap(0).start()
            for c in range(min(2, lent)):
                q_lend(c, 0).start()
                g_lend(c, 0).start()
            for c in range(lent, chunks):
                fetch(c)

        @pl.when(inner)
        def _():
            for c in order:
                fetch(c)
            q_swap(order[0]).start()

        lgacc[...] = jnp.zeros_like(lgacc)
        zero = jnp.zeros(part.shape[1:], BF16)

        def clear(i, c):
            part[i] = zero
            return c

        lax.fori_loop(0, chunks, clear, 0)
        for cond, buf, d, count in (
            (low, rzp, 0, chunks), (borrows_low, rzp, 1, lent),
            (high, rzm, line - 1, chunks), (borrows_high, rzm, line - 2, lent),
        ):
            @pl.when(cond)
            def _():
                for i in range(count):
                    buf[i, d] = jnp.zeros(buf.shape[2:], BF16)

        for k in FAR:
            @pl.when(gets_from(k))
            def _():
                la_copy(k).wait_recv()
                lb_copy(k).start()
                lc_copy(2 * (k + 1), core).start()

            @pl.when(jnp.logical_not(gets_from(k)))
            def _():
                for b in (2 * (k + 1), 2 * (k + 1) + 1):
                    lat_all[b] = jnp.zeros(lat_all.shape[1:], BF16)
        g_swap(0).start()
        la_copy(0).wait_recv()
        lc_copy(3, core).start()
        for k in FAR:
            @pl.when(gets_from(k))
            def _():
                lb_copy(k).wait_recv()
                lc_copy(2 * (k + 1) + 1, core).start()

        @pl.when(edge)
        def _():
            for c in range(max(lent, plain)):
                if c < plain:
                    swap(lent + c)
                if c + 1 < lent:
                    swap(c + 1)
            lend_mate(0)
            for c in range(2, lent):
                q_lend(c, 0).start()
                g_lend(c, 0).start()

        @pl.when(inner)
        def _():
            for c in order[1:]:
                swap(c)

        lc_copy(3, 1 - core).wait_recv()
        for k in FAR:
            @pl.when(gets_from(k))
            def _():
                lc_copy(2 * (k + 1), 1 - core).wait_recv()
                lc_copy(2 * (k + 1) + 1, 1 - core).wait_recv()
        for b in range(SPAN):
            rows = lat_all[b].reshape(tok, lat_all.shape[3])
            lat_t[:, b * tok:(b + 1) * tok] = jnp.transpose(rows[:, :LATENT])

        def ids_of(b):
            tail = lat_all[b].reshape(tok, lat_all.shape[3])[:, LATENT:].astype(F32)
            return jnp.transpose(tail)[ROPE:ROPE + 1, :]

        row = lax.broadcasted_iota(jnp.int32, (tok, tok), 0)
        col = lax.broadcasted_iota(jnp.int32, (tok, tok), 1)

        def mask(which, window, query_at, shift):
            for k in range(2):
                query_id = ids_of(query_at + k)
                for b in range(BLOCKS):
                    back = window // 2 - 1 + b // 2
                    block = (s if b % 2 == 0 else mate) - 2 * back
                    rows = lat_all[window + b].reshape(tok, lat_all.shape[3])
                    key_id = rows[:, width:width + 1].astype(F32)
                    first = (s if k == 0 else mate) + shift - block
                    visible = (row <= col + first * tok) & (block >= 0) & (key_id == query_id)
                    bias[which, b * tok:(b + 1) * tok, k * tok:(k + 1) * tok] = jnp.where(visible, 0.0, -jnp.inf)

        mask(0, 2, 2, 0)

        @pl.when(borrows_low)
        def _():
            mask(1, 2, 4, -2)

        @pl.when(borrows_high)
        def _():
            mask(1, 0, 0, 2)

    def compute(c, is_lent):
        slot = jnp.where(is_lent, chunks + c, c)
        which = jnp.where(is_lent, 1, 0)
        window = jnp.where(is_lent & borrows_high, 0, 2)

        @pl.when(jnp.logical_not(is_lent))
        def _():
            w_copy(c, 0).wait()
            w_copy(c, 1).wait()
            q_own(c).wait()
            g_own(c).wait()
            q_swap(c).wait_recv()
            g_swap(c).wait_recv()

        @pl.when(is_lent)
        def _():
            for k in range(2):
                q_lend(c, k).wait_recv()
                g_lend(c, k).wait_recv()

        rows = lat_all[pl.ds(window, BLOCKS)].reshape(keys, lat_all.shape[3])
        lat = rows[:, :LATENT]
        rope = rows[:, LATENT:width]
        w = wb[c]
        q2 = qb[slot].reshape(queries, QW)
        g2 = gb[slot].reshape(queries, GW)
        kv = dot(lat, w, 1, 0).astype(BF16)
        dks, dvs, rope_sum = [], [], None
        for a in range(PAIR):
            q = q2[:, a * (NOPE + ROPE):(a + 1) * (NOPE + ROPE)]
            g = g2[:, a * VDIM:(a + 1) * VDIM]
            v = kv[:, PAIR * NOPE + a * VDIM:PAIR * NOPE + (a + 1) * VDIM]
            k = jnp.concatenate([kv[:, a * NOPE:(a + 1) * NOPE], rope], axis=1)
            sc = dot(k, q, 1, 1) * (scale * to_log2) + bias[which]
            e = jnp.exp2(sc - jnp.max(sc, axis=0, keepdims=True))
            p = e * (1.0 / jnp.sum(e, axis=0, keepdims=True))
            pb = p.astype(BF16)
            att = jnp.transpose(dot(v, pb, 0, 0)).astype(BF16)
            for k in range(2):
                atts[slot, k, :, a * VDIM:(a + 1) * VDIM] = att[k * tok:(k + 1) * tok]
            dp = dot(v, g, 1, 1)
            delta = jnp.sum(p * dp, axis=0, keepdims=True)
            ds = (p * (dp - delta) * scale).astype(BF16)
            dk = dot(ds, q, 1, 0)
            dvs.append(dot(pb, g, 1, 0).astype(BF16))
            dks.append(dk[:, :NOPE].astype(BF16))
            r = dk[:, NOPE:]
            rope_sum = r if rope_sum is None else rope_sum + r
        dd = jnp.concatenate(dks + dvs, axis=1)
        lat_cols = lat_t[:, pl.ds(pl.multiple_of(window * tok, 128), keys)]
        grad = dot(lat_cols, dd, 1, 0).reshape(part.shape[1:])
        part[c] = (part[c].astype(F32) + grad).astype(BF16)
        flat = (BLOCKS,) + lgacc.shape[1:4]
        at = pl.ds(window, BLOCKS)
        lgacc[at, :, :, :, :LATENT] += dot(dd, w, 1, 1).reshape(*flat, LATENT)
        lgacc[at, :, :, :, LATENT:] += rope_sum.reshape(*flat, ROPE)

        @pl.when(is_lent)
        def _():
            for k in range(2):
                a_lent(c, k).start()

        @pl.when(jnp.logical_not(is_lent))
        def _():
            a_swap(c, y).start()
            att_ref[:, cols(y, c, GW)] = atts[c, 0]

    def pass_on(i, r, up, first):
        d = line - 1 - r if up else r

        @pl.when(jnp.logical_not(first))
        def _():
            z_copy(i, d, up).wait_recv()
            buf = rzp if up else rzm
            part[i, d] = (part[i, d].astype(F32) + buf[i, d].astype(F32)).astype(BF16)

        z_copy(i, d, up).start()

    def pass_range(i, r0, r1, up, first):
        def one(r, c):
            pass_on(i, r, up, first)
            return c

        lax.fori_loop(r0, r1, one, 0)

    def pass_late(k0, k1, up):
        def one(k, c):
            pass_on(chunks - late + k % late, k // late, up, True)
            return c

        lax.fori_loop(k0, k1, one, 0)

    def relay(j, up):
        pos = z if up else line - 1 - z
        reach = line - 1 - pos
        t = j - 2 * (pos - 1)

        @pl.when(pos == 0)
        def _():
            @pl.when(j < plain - late)
            def _():
                pass_range(lent + j, 0, line - 1, up, True)

            @pl.when(j == plain - 1)
            def _():
                pass_late(0, late * (line - 1), up)

        @pl.when(pos > 0)
        def _():
            lead = jnp.int32(0)
            for c in range(lent):
                lead = jnp.where(t == ready[c], c + 1, lead)

            @pl.when(lead > 0)
            def _():
                pass_range(lead - 1, 0, reach, up, pos == 1)

            near, nearer = jnp.int32(0), jnp.int32(0)
            for c in range(lent, chunks - late):
                near = jnp.where(t == ready[c], c + 1, near)
                nearer = jnp.where(t == ready[c] + 1, c + 1, nearer)

            @pl.when((near > 0) & (reach > 0))
            def _():
                pass_on(near - 1, 0, up, False)

            @pl.when(nearer > 0)
            def _():
                pass_range(nearer - 1, 1, reach, up, False)

            k = t - (work - 1)

            @pl.when((k >= 0) & (k < late * reach))
            def _():
                pass_on(chunks - late + k % late, k // late, up, False)

    def finish(i):
        @pl.when(jnp.logical_not(low) & jnp.logical_not(borrows_low & (i < lent)))
        def _():
            z_copy(i, z, True).wait_recv()

        @pl.when(jnp.logical_not(high) & jnp.logical_not(borrows_high & (i < lent)))
        def _():
            z_copy(i, z, False).wait_recv()

        def total(yy):
            return part[i, z, yy].astype(F32) + rzp[i, z, yy].astype(F32) + rzm[i, z, yy].astype(F32)

        part[i, z, other] = total(other).astype(BF16)
        y_copy(i).start()
        put(i, y, total(y))

    def put(i, half, rows):
        kwg_ref[:, cols(half, i, PAIR * NOPE)] = rows[:, :PAIR * NOPE]
        vwg_ref[:, cols(half, i, GW)] = rows[:, PAIR * NOPE:]

    def close(i, carry):
        y_copy(i).wait_recv()
        put(i, other, yr[i].astype(F32))
        return carry

    def latent_twin():
        l1s[...] = lgacc[:, :, 1 - core].astype(BF16)
        l1_copy().start()

    def latent_send():
        l1_copy().wait_recv()
        twos[...] = lgacc[:, :, core] + l1r[...].astype(F32)
        for k in range(1, chips):
            xs[k - 1] = twos[:, (chip + k) % chips].astype(BF16)
        for p in PAIRS:
            @pl.when(gets_from(p - 1))
            def _():
                for k in range(1, chips):
                    x_copy(k, p).start()

    def latent_pass():
        for p in PAIRS:
            @pl.when(gets_from(p - 1))
            def _():
                for k in range(1, chips):
                    x_copy(k, p).wait_recv()
                for b in (2 * p, 2 * p + 1):
                    tot = twos[b, chip]
                    for k in range(1, chips):
                        tot = tot + xr[k - 1, b].astype(F32)
                    if b == 2:
                        lgown[...] = tot
                    elif 2 * p == SPAN - 4:
                        @pl.when(borrows_high)
                        def _():
                            l2_copy(b + 2).wait_recv()
                            l2s[b] = (tot + l2r[b + 2].astype(F32)).astype(BF16)

                        @pl.when(jnp.logical_not(borrows_high))
                        def _():
                            l2s[b] = tot.astype(BF16)
                        l2_copy(b).start()
                    else:
                        l2s[b] = tot.astype(BF16)
                        l2_copy(b).start()

    def latent_gather():
        for b in range(SPAN):
            if b != 2:
                last_hop = z != line - 3 if b >= SPAN - 2 else z >= 0

                @pl.when(sends_to(b // 2 - 1) & last_hop)
                def _():
                    l2_copy(b).wait_recv()
                    lgown[...] += l2r[b].astype(F32)
        hb[h] = lgown[...].astype(BF16)
        for k in range(1, hn):
            h_copy(k, h).start()

    def latent_out():
        for k in range(1, hn):
            h_copy(k, (h + k) % hn).wait_recv()
        lg_ref[...] = jnp.transpose(hb[...].astype(F32).reshape(tok, width))

    enter()
    last = max(done.values()) + 1

    def turn(j, carry):
        c = jnp.where(edge, lent + j, pick([c for c, _ in turns], j))
        is_lent = inner & (pick([f for _, f in turns], j) > 0)
        active = (j < jnp.where(edge, plain, work)) & (borrows | jnp.logical_not(is_lent))

        @pl.when(active)
        def _():
            compute(c, is_lent)

        @pl.when(edge & (j < lent - 1))
        def _():
            lend_mate(j + 1)

        spent = jnp.where(edge, plain - 1, work - 1)

        @pl.when(j == spent)
        def _():
            latent_twin()

        @pl.when((j == spent + 1) & edge)
        def _():
            latent_send()

        @pl.when((j == spent + 2) & edge)
        def _():
            latent_pass()

        for up in (True, False):
            relay(j, up)

        @pl.when((j == spent + 1) & inner)
        def _():
            latent_send()

        @pl.when((j == spent + late * (line - 2) - 2) & inner)
        def _():
            latent_pass()

        fin = jnp.int32(0)
        for i in range(chunks):
            fin = jnp.where(j == done[i], i + 1, fin)

        @pl.when(fin > 0)
        def _():
            finish(fin - 1)

        @pl.when(edge & (fin > 0) & (fin <= lent))
        def _():
            for k in range(2):
                a_lent(fin - 1, k).wait_recv()
            a_swap(fin - 1, y).start()
            att_ref[:, cols(y, fin - 1, GW)] = atts[fin - 1, 0]

        @pl.when(j == last - late - 1)
        def _():
            lax.fori_loop(0, chunks - late, close, 0)

        return carry

    lax.fori_loop(0, last, turn, 0)
    latent_gather()
    lax.fori_loop(chunks - late, chunks, close, 0)
    latent_out()

    for k in range(1, hn):
        h_copy(k, h).wait_send()
    l1_copy().wait_send()
    for k in range(1, chips):
        for p in PAIRS:
            @pl.when(gets_from(p - 1))
            def _():
                x_copy(k, p).wait_send()
    for b in range(SPAN):
        if b != 2:
            @pl.when(gets_from(b // 2 - 1))
            def _():
                l2_copy(b).wait_send()

    def drain(j, carry):
        y_copy(j).wait_send()
        a_swap(j, other).wait_recv()
        a_swap(j, y).wait_send()
        q_swap(j).wait_send()
        g_swap(j).wait_send()
        for d in range(line):
            @pl.when((d > z) & jnp.logical_not(low & (j < lent)))
            def _():
                z_copy(j, d, True).wait_send()

            @pl.when((d < z) & jnp.logical_not(high & (j < lent)))
            def _():
                z_copy(j, d, False).wait_send()
        return carry

    lax.fori_loop(0, chunks, drain, 0)
    for c in range(lent):
        for k in range(2):
            @pl.when(edge)
            def _():
                q_lend(c, k).wait_send()
                g_lend(c, k).wait_send()

            @pl.when(borrows)
            def _():
                a_lent(c, k).wait_send()
    la_copy(0).wait_send()
    lc_copy(3, core).wait_send()
    for k in FAR:
        @pl.when(sends_to(k))
        def _():
            la_copy(k).wait_send()

        @pl.when(gets_from(k))
        def _():
            lb_copy(k).wait_send()
            lc_copy(2 * (k + 1), core).wait_send()
            lc_copy(2 * (k + 1) + 1, core).wait_send()


def flush(*refs):
    sems = refs[-1]
    copies = [pltpu.make_async_copy(refs[k], refs[4 + k], sems.at[k]) for k in range(4)]
    for copy in copies:
        copy.start()
    for copy in copies:
        copy.wait()


def per_device(n, hn, queries, latents, doc_ids, key_weight, value_weight, out_grad):
    tok = latents.shape[0]
    heads = key_weight.shape[1] // NOPE
    chunks = heads // 2 // PAIR
    line = n // 2
    rows = LATENT // n
    lent = plan(chunks, line)[0]
    slots = chunks + lent
    keys = BLOCKS * tok
    width = LATENT + ROPE
    wide = width + 64
    share = tok // hn
    chips = hn // 2
    ids = doc_ids.reshape(1, tok)
    whole = pl.BlockSpec(memory_space=pltpu.VMEM)
    far = pl.BlockSpec(memory_space=pltpu.HBM)
    dma = pltpu.SemaphoreType.DMA
    ring = max(chips - 1, 1)
    att, lg, kwg, vwg = pl.pallas_call(
        functools.partial(kernel, n, hn, chunks),
        out_shape=(
            pltpu.VMEM((tok, heads * VDIM), BF16),
            pltpu.VMEM((width, tok), F32),
            pltpu.VMEM((rows, heads * NOPE), F32),
            pltpu.VMEM((rows, heads * VDIM), F32),
        ),
        in_specs=[far] * 6,
        out_specs=(whole, whole, whole, whole),
        scratch_shapes=[
            pltpu.VMEM((width, tok), BF16),
            pltpu.VMEM((1, tok), jnp.int32),
            pltpu.VMEM((SPAN, 2, tok // 2, wide), BF16),
            pltpu.VMEM((LATENT, SPAN * tok), BF16),
            pltpu.VMEM((2, keys, 2 * tok), F32),
            pltpu.VMEM((SPAN, chips, 2, share, width), F32),
            pltpu.VMEM((chunks, LATENT, WW), BF16),
            pltpu.VMEM((slots, 2, tok, QW), BF16),
            pltpu.VMEM((slots, 2, tok, GW), BF16),
            pltpu.VMEM((slots, 2, tok, GW), BF16),
            pltpu.VMEM((chunks, line, 2, rows, WW), BF16),
            pltpu.VMEM((chunks, line, 2, rows, WW), BF16),
            pltpu.VMEM((chunks, line, 2, rows, WW), BF16),
            pltpu.VMEM((chunks, rows, WW), BF16),
            pltpu.VMEM((SPAN, chips, share, width), BF16),
            pltpu.VMEM((SPAN, chips, share, width), BF16),
            pltpu.VMEM((SPAN, chips, share, width), F32),
            pltpu.VMEM((ring, SPAN, share, width), BF16),
            pltpu.VMEM((ring, SPAN, share, width), BF16),
            pltpu.VMEM((SPAN, share, width), BF16),
            pltpu.VMEM((SPAN, share, width), BF16),
            pltpu.VMEM((share, width), F32),
            pltpu.VMEM((hn, share, width), BF16),
            dma((2,)), dma((chunks, 2)), dma((chunks,)), dma((chunks,)),
            dma((chunks,)), dma((chunks,)), dma((chunks,)), dma((chunks,)),
            dma((lent, 2)), dma((lent, 2)), dma((lent, 2)), dma((lent, 2)),
            dma((slots, 2)), dma((chunks,)), dma((lent, 2)),
            dma((BACK + 2,)), dma((BACK + 2,)), dma((BACK + 2,)), dma((BACK + 2,)), dma((SPAN,)), dma((SPAN,)),
            dma((chunks, line)), dma((chunks, line)), dma((chunks, line)), dma((chunks, line)),
            dma((chunks,)), dma((chunks,)),
            dma((1,)), dma((1,)), dma((ring, SPAN // 2)), dma((ring, SPAN // 2)), dma((SPAN,)), dma((SPAN,)),
            dma((max(hn - 1, 1),)), dma((hn,)),
        ],
        compiler_params=pltpu.CompilerParams(
            collective_id=0,
            has_side_effects=True,
            vmem_limit_bytes=VMEM_LIMIT,
        ),
    )(latents.T, ids, queries, out_grad, key_weight, value_weight)
    out = (att, lg, kwg, vwg)
    att, lg, kwg, vwg = pl.pallas_call(
        flush,
        out_shape=tuple(pltpu.HBM(o.shape, o.dtype) for o in out),
        in_specs=[whole] * 4,
        out_specs=(far,) * 4,
        scratch_shapes=[dma((4,))],
        compiler_params=pltpu.CompilerParams(vmem_limit_bytes=1024 * 1024),
    )(*out)
    return att, lg.T, kwg, vwg


def solution(mesh):
    in_specs = (
        P("seq", "head"),
        P("seq", None),
        P("seq"),
        P(None, "head"),
        P(None, "head"),
        P("seq", "head"),
    )
    out_specs = (P("seq", "head"), P("seq", None), P("seq", "head"), P("seq", "head"))
    body = functools.partial(per_device, mesh.shape["seq"], mesh.shape["head"])
    return jax.shard_map(
        body, mesh=mesh, in_specs=in_specs, out_specs=out_specs, check_vma=False
    )
```
